256 devices in a mesh: ctx: 64 (over z, y, core), head: 4 (over x).
Axes of the slice: x: 4, y: 4, z: 8, core: 2. Of those that a mesh axis runs over, the one named last changes fastest.
Arguments:
- queries: bfloat16 [16384, 4096], P(('ctx', 'head')), may hold values from -6.5 to 6.5
- keys: bfloat16 [16384, 2048], P(('ctx', 'head')), may hold values from -6.5 to 6.5
- values: bfloat16 [16384, 2048], P(('ctx', 'head')), may hold values from -6 to 6
- grad_out: bfloat16 [16384, 4096], P(('ctx', 'head')), may hold values from -6 to 6
- segments: int32 [16384], P('ctx'), may hold values from 0 to 7, never falling along the last dimension, each value on 1 to 4096 neighbouring positions
Outputs:
- attended: bfloat16 [16384, 4096], P(('ctx', 'head'))
- grad_queries: bfloat16 [16384, 4096], P(('ctx', 'head'))
- grad_keys: bfloat16 [16384, 2048], P(('ctx', 'head'))
- grad_values: bfloat16 [16384, 2048], P(('ctx', 'head'))
The draws below stay inside these ranges and needn't reach their ends.
Inputs may be any that keep to these rules, and one draw needn't show every extreme that they name: `segments`: document numbers never fall along the sequence; each document holds 1 to 4096 tokens.
All inputs are finite; a program needn't handle non-finite values.
Results may differ from the reference program's by a relative error of at most 0.019.
Values may be sent and summed in bfloat16 or wider, within the bound.
A program may use at most 64 MiB of HBM per device.

```python
import math
import jax
import jax.numpy as jnp
import numpy as np
from jax import lax

QHEADS = 32
KVHEADS = 16
HEAD_DIM = 128
WINDOW = 1024
TOKENS = 16384
DOCS = 8
DOC_MOST = 4096


def base_rows(key, width, salt):
    sample_key = jax.random.fold_in(jax.random.fold_in(key, salt), 0)
    return jnp.clip(jax.random.normal(sample_key, (TOKENS, width), jnp.float32), -6.0, 6.0)


def draw_queries(key, part):
    drawn = base_rows(key, QHEADS * HEAD_DIM, 11)
    return drawn.astype(jnp.bfloat16)


def draw_keys(key, part):
    drawn = base_rows(key, KVHEADS * HEAD_DIM, 23)
    return drawn.astype(jnp.bfloat16)


def block_scale(stream_key, dims, cuts, least, high):
    level = 1.0
    for dim, blocks in cuts:
        steps = jax.random.uniform(jax.random.fold_in(jax.random.fold_in(stream_key, 6), dim), (blocks,), jnp.float32, least / len(cuts), high / len(cuts))
        level = level * jnp.repeat(jnp.exp(steps), dims[dim] // blocks).reshape((-1,) + (1,) * (len(dims) - 1 - dim))
    return level


def split_up(count, total, reach, skew):
    loads = [(1 << 20) // math.isqrt(rank ** skew) + 1 for rank in range(2, count + 1)]
    spare, counts = total - reach - (count - 1), [1] * (count - 1)
    while spare > 0:
        candidates = [i for i in range(count - 1) if counts[i] < reach]
        whole, left = sum([loads[i] for i in candidates]), spare
        for i in candidates:
            more = min(reach - counts[i], max(1, left * loads[i] // whole), spare)
            counts[i] = counts[i] + more
            spare = spare - more
    return np.array([reach] + counts)


def ragged_sizes(key, count, total, bound, slope):
    if count == 2:
        one = jax.random.randint(key, (), max(1, total - bound), min(bound, total - 1) + 1)
        return jnp.stack([one, total - one])
    tallies = jnp.asarray(split_up(count, total, bound, slope), jnp.int32)
    twos = (count - 1) // 2
    source_of, receiver = tallies[1:1 + 2 * twos:2], tallies[2:2 + 2 * twos:2]
    slack = jnp.minimum(source_of - 1, bound - receiver)
    passed = jax.random.randint(jax.random.fold_in(key, 1), (twos,), 0, 1 << 20) % (slack + 1)
    tallies = tallies.at[1:1 + 2 * twos:2].set(source_of - passed).at[2:2 + 2 * twos:2].set(receiver + passed)
    return tallies[jax.random.permutation(jax.random.fold_in(key, 2), count)]


def noise(stream_key, extent, deviation, most, shards=(), kind=jnp.bfloat16):
    values = jax.random.normal(stream_key, extent, jnp.float32) * deviation
    if len(shards) > 0:
        values = block_scale(stream_key, extent, shards, -0.22, 0.18) * values
    return jnp.clip(values, min=-most, max=most).astype(kind)


def setup_inputs(seed: int = 0) -> dict:
    splits = jax.random.split(jax.random.key(seed), 6)
    queries = draw_queries(jax.random.fold_in(splits[5], 71), 0)
    keys = draw_keys(jax.random.fold_in(splits[5], 71), 0)
    values = noise(splits[2], (TOKENS, KVHEADS * HEAD_DIM), 1.0, 6.0, ((0, 256),))
    grad_out = noise(splits[3], (TOKENS, QHEADS * HEAD_DIM), 1.0, 6.0, ((0, 256),))
    segments = jnp.searchsorted(jnp.cumsum(ragged_sizes(splits[4], DOCS, TOKENS, DOC_MOST, 2)), jnp.arange(TOKENS), side="right").astype(jnp.int32)
    return dict(queries=queries, keys=keys, values=values, grad_out=grad_out, segments=segments)


ATTN_SCALE = 168.0 ** -0.5
HIGHEST = lax.Precision.HIGHEST


def window_mask(query_ids, key_ids, query_pos, key_pos):
    distance = query_pos[:, None] - key_pos[None, :]
    return (query_ids[:, None] == key_ids[None, :]) & (distance >= 0) & (distance < WINDOW)


def to_low(array):
    return lax.optimization_barrier(array.astype(jnp.bfloat16)).astype(jnp.float32)


def reference(queries, keys, values, grad_out, segments):
    per_group = QHEADS // KVHEADS
    block_count = TOKENS // WINDOW
    query_heads = queries.reshape(TOKENS, KVHEADS, per_group, HEAD_DIM)
    grad_heads = grad_out.reshape(TOKENS, KVHEADS, per_group, HEAD_DIM)
    key_heads = keys.reshape(TOKENS, KVHEADS, HEAD_DIM)
    value_heads = values.reshape(TOKENS, KVHEADS, HEAD_DIM)
    blank_pairs = jnp.zeros((WINDOW, KVHEADS, HEAD_DIM), jnp.bfloat16)
    padded_keys = jnp.concatenate((blank_pairs, key_heads), 0)
    padded_values = jnp.concatenate((blank_pairs, value_heads), 0)
    blank_ids = jnp.full((WINDOW,), -1, jnp.int32)
    padded_ids = jnp.concatenate((blank_ids, segments), 0)
    positions = jnp.arange(WINDOW, dtype=jnp.int32)
    key_span = jnp.arange(2 * WINDOW, dtype=jnp.int32)

    def forward_block(block_index):
        start = (block_index * WINDOW).astype(jnp.int32)
        block_queries = lax.dynamic_slice_in_dim(query_heads, start, WINDOW, 0).astype(jnp.float32)
        block_grads = lax.dynamic_slice_in_dim(grad_heads, start, WINDOW, 0).astype(jnp.float32)
        near_keys = lax.dynamic_slice_in_dim(padded_keys, start, 2 * WINDOW, 0).astype(jnp.float32)
        near_values = lax.dynamic_slice_in_dim(padded_values, start, 2 * WINDOW, 0).astype(jnp.float32)
        query_ids = lax.dynamic_slice_in_dim(segments, start, WINDOW, 0)
        key_ids = lax.dynamic_slice_in_dim(padded_ids, start, 2 * WINDOW, 0)
        visible = window_mask(query_ids, key_ids, positions + WINDOW, key_span)
        scores = jnp.einsum("agnd,cgd->gnac", block_queries, near_keys, precision=HIGHEST) * ATTN_SCALE
        masked = jnp.where(visible[None, None], scores, -jnp.inf)
        highest = jnp.max(masked, axis=3, keepdims=True)
        weights = jnp.exp(masked - highest)
        totals = jnp.sum(weights, axis=3, keepdims=True)
        probs = weights / totals
        logsum = (highest + jnp.log(totals))[..., 0]
        probs_low = to_low(probs)
        outputs = jnp.einsum("gnac,cgd->agnd", probs_low, near_values, precision=HIGHEST).astype(jnp.bfloat16)
        delta = jnp.sum(outputs.astype(jnp.float32) * block_grads, axis=3)
        prob_grads = jnp.einsum("agnd,cgd->gnac", block_grads, near_values, precision=HIGHEST)
        score_grads = to_low(ATTN_SCALE * probs * (prob_grads - jnp.transpose(delta, (1, 2, 0))[..., None]))
        query_grads = jnp.einsum("gnac,cgd->agnd", score_grads, near_keys, precision=HIGHEST).astype(jnp.bfloat16)
        return outputs, query_grads, logsum, delta

    block_ids = jnp.arange(block_count, dtype=jnp.int32)
    outputs, query_grads, logsum, delta = lax.map(forward_block, block_ids)
    attended = outputs.reshape(TOKENS, QHEADS * HEAD_DIM)
    grad_queries = query_grads.reshape(TOKENS, QHEADS * HEAD_DIM)
    logsum_all = jnp.transpose(logsum, (0, 3, 1, 2)).reshape(TOKENS, KVHEADS, per_group)
    delta_all = delta.reshape(TOKENS, KVHEADS, per_group)

    blank_queries = jnp.zeros((WINDOW, KVHEADS, per_group, HEAD_DIM), jnp.bfloat16)
    later_queries = jnp.concatenate((query_heads, blank_queries), 0)
    later_grads = jnp.concatenate((grad_heads, blank_queries), 0)
    later_ids = jnp.concatenate((segments, blank_ids), 0)
    blank_stats = jnp.zeros((WINDOW, KVHEADS, per_group), jnp.float32)
    later_logsum = jnp.concatenate((logsum_all, blank_stats), 0)
    later_delta = jnp.concatenate((delta_all, blank_stats), 0)

    def backward_block(block_index):
        start = (block_index * WINDOW).astype(jnp.int32)
        own_keys = lax.dynamic_slice_in_dim(key_heads, start, WINDOW, 0).astype(jnp.float32)
        own_values = lax.dynamic_slice_in_dim(value_heads, start, WINDOW, 0).astype(jnp.float32)
        block_queries = lax.dynamic_slice_in_dim(later_queries, start, 2 * WINDOW, 0).astype(jnp.float32)
        block_grads = lax.dynamic_slice_in_dim(later_grads, start, 2 * WINDOW, 0).astype(jnp.float32)
        key_ids = lax.dynamic_slice_in_dim(segments, start, WINDOW, 0)
        query_ids = lax.dynamic_slice_in_dim(later_ids, start, 2 * WINDOW, 0)
        visible = window_mask(query_ids, key_ids, key_span, positions)
        scores = jnp.einsum("agnd,cgd->gnac", block_queries, own_keys, precision=HIGHEST) * ATTN_SCALE
        block_logsum = jnp.transpose(lax.dynamic_slice_in_dim(later_logsum, start, 2 * WINDOW, 0), (1, 2, 0))
        block_delta = jnp.transpose(lax.dynamic_slice_in_dim(later_delta, start, 2 * WINDOW, 0), (1, 2, 0))
        probs = jnp.where(visible[None, None], jnp.exp(scores - block_logsum[..., None]), 0.0)
        probs_low = to_low(probs)
        value_grads = jnp.einsum("gnac,agnd->cgd", probs_low, block_grads, precision=HIGHEST).astype(jnp.bfloat16)
        prob_grads = jnp.einsum("agnd,cgd->gnac", block_grads, own_values, precision=HIGHEST)
        score_grads = to_low(ATTN_SCALE * probs * (prob_grads - block_delta[..., None]))
        key_grads = jnp.einsum("gnac,agnd->cgd", score_grads, block_queries, precision=HIGHEST).astype(jnp.bfloat16)
        return key_grads, value_grads

    key_grads, value_grads = lax.map(backward_block, block_ids)
    grad_keys = key_grads.reshape(TOKENS, KVHEADS * HEAD_DIM)
    grad_values = value_grads.reshape(TOKENS, KVHEADS * HEAD_DIM)
    return attended, grad_queries, grad_keys, grad_values
```

```python
import functools
import math

import jax
import jax.numpy as jnp
from jax import lax
from jax.experimental import pallas as pl
from jax.experimental.pallas import tpu as pltpu
from jax.sharding import PartitionSpec as P

QHEADS = 32
KVHEADS = 16
HEAD_DIM = 128
WINDOW = 1024
DOCS = 8

ATTN_SCALE = 168.0 ** (-0.5)
EXP2_SCALE = ATTN_SCALE * math.log2(math.e)
MESH = pl.DeviceIdType.MESH

ROWS = 64
TILE = 256
STEPS = WINDOW // TILE
SPAN = WINDOW + TILE
PAIR = 2 * HEAD_DIM
HIDDEN = -1e30


def dot(a, b, dims=((1,), (0,))):
    return lax.dot_general(a, b, (dims, ((), ())), preferred_element_type=jnp.float32)


def await_bytes(ref, sem):
    pltpu.make_async_copy(ref, ref, sem).wait()


def kernel(
    q_ref, k_ref, v_ref, g_ref, seg_ref,
    a_ref, gq_ref, gk_ref, gv_ref,
    qb, kb, vb, gb, segb,
    kt, vt, pb, ot, lo_buf, ab, gqb, dk_acc, dv_acc, dk_out, dv_out, dk_in, dv_in, gkb, gvb,
    send, recv, ring_send, ring_recv, out_send, out_recv,
):
    ctx, x = lax.axis_index("ctx"), lax.axis_index("head")
    core, y, z = ctx % 2, (ctx // 2) % 4, ctx // 8
    planes = lax.axis_size("ctx") // 8
    half = y // 2
    slot = ((y % 2) * 2 + core) * 4 + x
    group = x * 4 + y
    after = (jnp.where(core == 0, ctx + 1, ((z + 1) % planes) * 8 + y * 2), x)
    before = (jnp.where(core == 1, ctx - 1, ((z + planes - 1) % planes) * 8 + y * 2 + 1), x)
    stays = half == core

    def source(yy, c, dx):
        return ((z * 4 + core * 2 + yy) * 2 + c, (x + dx) % 4)

    barrier = pltpu.get_barrier_semaphore()
    for yy in range(2):
        for c in range(2):
            for dx in range(4):
                pl.semaphore_signal(barrier, inc=1, device_id=source(yy, c, dx), device_id_type=MESH)
    pl.semaphore_signal(barrier, inc=1, device_id=before, device_id_type=MESH)
    pl.semaphore_wait(barrier, 17)

    def target(dx, dy):
        tx, ty = (x + dx) % 4, (y + dy) % 4
        return ((z * 4 + ty) * 2 + half, tx), tx * 4 + ty

    def ship(src, dst, send_sem, recv_sem, where, local):
        def far():
            pltpu.make_async_remote_copy(
                src_ref=src, dst_ref=dst, send_sem=send_sem, recv_sem=recv_sem,
                device_id=where, device_id_type=MESH,
            ).start()

        if local is None:
            far()
        else:
            pl.when(local)(lambda: pltpu.make_async_copy(src, dst, recv_sem).start())
            pl.when(jnp.logical_not(local))(far)

    offsets = [(dx, dy) for dx in (2, 1, 3, 0) for dy in (2, 1, 3, 0)]
    own_rows = pl.ds(pl.multiple_of(slot * ROWS, ROWS), ROWS)
    own_rows2 = pl.ds(pl.multiple_of(WINDOW + slot * ROWS, ROWS), ROWS)
    for dy in range(4):
        where, _ = target(0, dy)
        ship(
            seg_ref, segb.at[STEPS + (y % 2) * 2 + core], send.at[4], recv.at[4],
            where, stays if dy == 0 else None,
        )
    for index, (src, dst, width, rows) in enumerate(
        (
            (k_ref, kb, HEAD_DIM, own_rows2),
            (v_ref, vb, HEAD_DIM, own_rows2),
            (q_ref, qb, PAIR, own_rows),
            (g_ref, gb, PAIR, own_rows),
        )
    ):
        for dx, dy in offsets:
            where, head = target(dx, dy)
            ship(
                src.at[:, pl.ds(pl.multiple_of(head * width, width), width)],
                dst.at[rows, :],
                send.at[index],
                recv.at[index],
                where,
                stays if dx == 0 and dy == 0 else None,
            )

    newer, older = pl.ds(WINDOW, WINDOW), pl.ds(0, WINDOW)
    ring = []
    for index, (buf, here, there) in enumerate(
        (
            (segb, pl.ds(STEPS, STEPS), pl.ds(0, STEPS)),
            (kb, newer, older),
            (vb, newer, older),
        )
    ):
        await_bytes(buf.at[here], recv.at[(4, 0, 1)[index]])
        copy = pltpu.make_async_remote_copy(
            src_ref=buf.at[here], dst_ref=buf.at[there],
            send_sem=ring_send.at[index], recv_sem=ring_recv.at[index],
            device_id=after, device_id_type=MESH,
        )
        copy.start()
        ring.append(copy)

    ring[0].wait()
    rows = [segb[r].astype(jnp.float32) for r in range(2 * STEPS)]
    for r in range(STEPS):
        rows[r] = jnp.where(ctx < 0, rows[r], jnp.where((z == 0) & (core == 0), -1.0, rows[r]))
    all_rows = jnp.concatenate(rows, axis=0)
    starts = [
        jnp.sum(
            jnp.sum((all_rows < d).astype(jnp.float32), axis=0, keepdims=True), axis=1, keepdims=True
        )
        for d in range(DOCS)
    ]
    lane = lax.broadcasted_iota(jnp.int32, (1, TILE), 1).astype(jnp.float32)
    for i in range(STEPS):
        row = rows[STEPS + i]
        first = jnp.maximum(lane + (i * TILE + 1.0), 0.0)
        for d in range(DOCS):
            first = jnp.maximum(first, jnp.where(row >= d, starts[d], 0.0))
        lo_buf[i] = (first - i * TILE).astype(jnp.int32)

    dk_acc[...] = jnp.zeros_like(dk_acc)
    dv_acc[...] = jnp.zeros_like(dv_acc)
    ring[1].wait()
    kt[...] = kb[...].T
    ring[2].wait()
    vt[...] = vb[...].T
    await_bytes(qb, recv.at[2])

    key_index = lax.broadcasted_iota(jnp.int32, (SPAN, TILE), 0)
    last_key = WINDOW + lax.broadcasted_iota(jnp.int32, (1, TILE), 1)

    def forward(i, carry):
        base = pl.multiple_of(i * TILE, TILE)
        keys = kb[pl.ds(base, SPAN), :]
        values_t = vt[:, pl.ds(base, SPAN)]
        seen = (key_index >= lo_buf[i]) & (key_index <= last_key)
        for n in range(2):
            columns = slice(n * HEAD_DIM, (n + 1) * HEAD_DIM)
            scores = dot(keys, qb[pl.ds(base, TILE), columns], ((1,), (1,)))
            scores = jnp.where(seen, scores, HIDDEN)
            top = jnp.max(scores, axis=0, keepdims=True)
            weights = jnp.exp2(scores * EXP2_SCALE - top * EXP2_SCALE)
            total = jnp.sum(weights, axis=0, keepdims=True)
            probs = (weights * (1.0 / total)).astype(jnp.bfloat16)
            pb[i, :, n * TILE : (n + 1) * TILE] = probs
            out_t = dot(values_t, probs)
            ot[n, i] = out_t
            ab[pl.ds(base, TILE), columns] = out_t.T.astype(jnp.bfloat16)
        for dx in range(4):
            send_back(ab, a_ref, PAIR, i, dx, 0)
        return carry

    def send_back(buf, out, width, i, dx, index):
        yy, c = i // 2, i % 2
        tx = (x + dx) % 4
        ty = core * 2 + yy
        where = ((z * 4 + ty) * 2 + c, tx)
        ship(
            buf.at[pl.ds(pl.multiple_of((i * 4 + tx) * ROWS, ROWS), ROWS), :],
            out.at[:, pl.ds(pl.multiple_of(group * width, width), width)],
            out_send.at[index],
            out_recv.at[index],
            where,
            ((ty == y) & (c == core)) if dx == 0 else None,
        )

    lax.fori_loop(0, STEPS, forward, 0)
    await_bytes(gb, recv.at[3])

    def backward(i, carry):
        base = pl.multiple_of(i * TILE, TILE)
        span = pl.ds(base, SPAN)
        values = vb[span, :]
        parts = []
        for n in range(2):
            columns = slice(n * HEAD_DIM, (n + 1) * HEAD_DIM)
            probs = pb[i, :, n * TILE : (n + 1) * TILE]
            grads_t = gb[pl.ds(base, TILE), columns].T
            low = ot[n, i].astype(jnp.bfloat16).astype(jnp.float32)
            delta = jnp.sum(low * grads_t.astype(jnp.float32), axis=0, keepdims=True)
            prob_grads = dot(values, grads_t)
            score_grads = (probs.astype(jnp.float32) * (prob_grads - delta)).astype(jnp.bfloat16)
            dq_t = dot(kt[:, span], score_grads) * ATTN_SCALE
            gqb[pl.ds(base, TILE), columns] = dq_t.T.astype(jnp.bfloat16)
            dv_acc[span, :] += dot(probs, gb[pl.ds(base, TILE), columns])
            dk_acc[span, :] += dot(score_grads, qb[pl.ds(base, TILE), columns])
        for dx in range(4):
            send_back(gqb, gq_ref, PAIR, i, dx, 1)
        return carry

    lax.fori_loop(0, STEPS, backward, 0)

    dk_out[...] = (dk_acc[older, :] * ATTN_SCALE).astype(jnp.bfloat16)
    dv_out[...] = dv_acc[older, :].astype(jnp.bfloat16)
    back = []
    for index, (src, dst) in enumerate(((dk_out, dk_in), (dv_out, dv_in))):
        copy = pltpu.make_async_remote_copy(
            src_ref=src, dst_ref=dst, send_sem=ring_send.at[3 + index], recv_sem=ring_recv.at[3 + index],
            device_id=before, device_id_type=MESH,
        )
        copy.start()
        back.append(copy)
    back[0].wait()
    gkb[...] = (dk_acc[newer, :] * ATTN_SCALE + dk_in[...].astype(jnp.float32)).astype(jnp.bfloat16)
    for i in range(STEPS):
        for dx in range(4):
            send_back(gkb, gk_ref, HEAD_DIM, i, dx, 2)
    back[1].wait()
    gvb[...] = (dv_acc[newer, :] + dv_in[...].astype(jnp.float32)).astype(jnp.bfloat16)
    for i in range(STEPS):
        for dx in range(4):
            send_back(gvb, gv_ref, HEAD_DIM, i, dx, 3)

    for index, out in enumerate((a_ref, gq_ref, gk_ref, gv_ref)):
        await_bytes(out, out_recv.at[index])
    for index, ref in enumerate((k_ref, v_ref, q_ref, g_ref)):
        width = ref.shape[1] // 16
        await_bytes(ref.at[:, pl.ds(0, 15 * width)], send.at[index])
        pl.when(jnp.logical_not(stays))(
            functools.partial(await_bytes, ref.at[:, pl.ds(0, width)], send.at[index])
        )
    for _ in range(3):
        await_bytes(seg_ref, send.at[4])
    pl.when(jnp.logical_not(stays))(functools.partial(await_bytes, seg_ref, send.at[4]))
    for index, buf in enumerate((ab, gqb, gkb, gvb)):
        await_bytes(buf.at[pl.ds(0, 15 * ROWS), :], out_send.at[index])
        pl.when(jnp.logical_not(stays))(
            functools.partial(await_bytes, buf.at[pl.ds(0, ROWS), :], out_send.at[index])
        )


def body(queries, keys, values, grad_out, segments):
    low = jnp.bfloat16
    shape = jax.ShapeDtypeStruct
    return pl.pallas_call(
        kernel,
        out_shape=(
            shape(queries.shape, low),
            shape(queries.shape, low),
            shape(keys.shape, low),
            shape(keys.shape, low),
        ),
        in_specs=[pl.BlockSpec(memory_space=pltpu.VMEM)] * 5,
        out_specs=[pl.BlockSpec(memory_space=pltpu.VMEM)] * 4,
        scratch_shapes=[
            pltpu.VMEM((WINDOW, PAIR), low),
            pltpu.VMEM((2 * WINDOW, HEAD_DIM), low),
            pltpu.VMEM((2 * WINDOW, HEAD_DIM), low),
            pltpu.VMEM((WINDOW, PAIR), low),
            pltpu.VMEM((2 * STEPS, 1, TILE), jnp.int32),
            pltpu.VMEM((HEAD_DIM, 2 * WINDOW), low),
            pltpu.VMEM((HEAD_DIM, 2 * WINDOW), low),
            pltpu.VMEM((STEPS, SPAN, 2 * TILE), low),
            pltpu.VMEM((2, STEPS, HEAD_DIM, TILE), jnp.float32),
            pltpu.VMEM((STEPS, 1, TILE), jnp.int32),
            pltpu.VMEM((WINDOW, PAIR), low),
            pltpu.VMEM((WINDOW, PAIR), low),
            pltpu.VMEM((2 * WINDOW, HEAD_DIM), jnp.float32),
            pltpu.VMEM((2 * WINDOW, HEAD_DIM), jnp.float32),
            pltpu.VMEM((WINDOW, HEAD_DIM), low),
            pltpu.VMEM((WINDOW, HEAD_DIM), low),
            pltpu.VMEM((WINDOW, HEAD_DIM), low),
            pltpu.VMEM((WINDOW, HEAD_DIM), low),
            pltpu.VMEM((WINDOW, HEAD_DIM), low),
            pltpu.VMEM((WINDOW, HEAD_DIM), low),
            pltpu.SemaphoreType.DMA((5,)),
            pltpu.SemaphoreType.DMA((5,)),
            pltpu.SemaphoreType.DMA((5,)),
            pltpu.SemaphoreType.DMA((5,)),
            pltpu.SemaphoreType.DMA((4,)),
            pltpu.SemaphoreType.DMA((4,)),
        ],
        compiler_params=pltpu.CompilerParams(
            collective_id=0, has_side_effects=True, vmem_limit_bytes=56 * 1024 * 1024
        ),
    )(queries, keys, values, grad_out, segments.reshape(1, TILE))


def solution(mesh):
    spec = P(("ctx", "head"), None)
    return jax.shard_map(
        body,
        mesh=mesh,
        in_specs=(spec, spec, spec, spec, P("ctx")),
        out_specs=(spec, spec, spec, spec),
        check_vma=False,
    )
```

```python
import functools
import math

import jax
import jax.numpy as jnp
from jax import lax
from jax.experimental import pallas as pl
from jax.experimental.pallas import tpu as pltpu
from jax.sharding import PartitionSpec as P

QHEADS = 32
KVHEADS = 16
HEAD_DIM = 128
WINDOW = 1024
DOCS = 8

ATTN_SCALE = 168.0 ** (-0.5)
EXP2_SCALE = ATTN_SCALE * math.log2(math.e)
MESH = pl.DeviceIdType.MESH

ROWS = 64
TILE = 256
STEPS = WINDOW // TILE
SPAN = WINDOW + TILE
HIDDEN = -1e30


def dot(a, b, dims=((1,), (0,))):
    return lax.dot_general(a, b, (dims, ((), ())), preferred_element_type=jnp.float32)


def await_bytes(ref, sem):
    pltpu.make_async_copy(ref, ref, sem).wait()


def kernel(
    q_ref, k_ref, v_ref, g_ref, seg_ref,
    a_ref, gq_ref, gk_ref, gv_ref,
    q_own, k_own, v_own, g_own,
    qb, kb, vb, gb, segb,
    kt, vt, pb, ot, dq, lo_buf, ab, gqb, dk_acc, dv_acc, dk_out, dv_out, dk_in, dv_in, gkb, gvb,
    load, send, recv, ring_send, ring_recv, out_send, out_recv,
):
    ctx, x = lax.axis_index("ctx"), lax.axis_index("head")
    core, y, z = ctx % 2, (ctx // 2) % 4, ctx // 8
    planes = lax.axis_size("ctx") // 8
    half = y // 2
    slot = ((y % 2) * 2 + core) * 4 + x
    group = x * 4 + y
    has_after = (z < planes - 1) | (core == 0)
    has_before = (z > 0) | (core == 1)
    after = (jnp.where(core == 0, ctx + 1, ((z + 1) % planes) * 8 + y * 2), x)
    before = (jnp.where(core == 1, ctx - 1, ((z + planes - 1) % planes) * 8 + y * 2 + 1), x)
    stays = half == core
    leaves = jnp.logical_not(stays)

    def source(yy, c, dx):
        return ((z * 4 + core * 2 + yy) * 2 + c, (x + dx) % 4)

    barrier = pltpu.get_barrier_semaphore()
    for yy in range(2):
        for c in range(2):
            for dx in range(4):
                pl.semaphore_signal(barrier, inc=1, device_id=source(yy, c, dx), device_id_type=MESH)

    @pl.when(has_before)
    def _():
        pl.semaphore_signal(barrier, inc=1, device_id=before, device_id_type=MESH)

    loads = [
        pltpu.make_async_copy(src, dst, load.at[n])
        for n, (src, dst) in enumerate(
            ((k_ref, k_own), (v_ref, v_own), (q_ref, q_own), (g_ref, g_own))
        )
    ]
    for copy in loads:
        copy.start()
    newer, older = pl.ds(WINDOW, WINDOW), pl.ds(0, WINDOW)

    @pl.when(jnp.logical_not(has_before))
    def _():
        kb[older, :] = jnp.zeros((WINDOW, HEAD_DIM), kb.dtype)
        vb[older, :] = jnp.zeros((WINDOW, HEAD_DIM), vb.dtype)
        segb[pl.ds(0, STEPS)] = jnp.full((STEPS, 1, TILE), -1, segb.dtype)

    pl.semaphore_wait(barrier, 16 + has_after.astype(jnp.int32))

    def target(dx, dy):
        tx, ty = (x + dx) % 4, (y + dy) % 4
        return ((z * 4 + ty) * 2 + half, tx), tx * 4 + ty

    def ship(src, dst, send_sem, recv_sem, where, local):
        def far():
            pltpu.make_async_remote_copy(
                src_ref=src, dst_ref=dst, send_sem=send_sem, recv_sem=recv_sem,
                device_id=where, device_id_type=MESH,
            ).start()

        if local is None:
            far()
        else:
            pl.when(local)(lambda: pltpu.make_async_copy(src, dst, recv_sem).start())
            pl.when(jnp.logical_not(local))(far)

    offsets = [(dx, dy) for dx in range(4) for dy in range(4)]
    offsets = sorted(offsets, key=lambda o: min(o[0], 4 - o[0]) + min(o[1], 4 - o[1]))
    own_rows = pl.ds(pl.multiple_of(slot * ROWS, ROWS), ROWS)
    own_rows2 = pl.ds(pl.multiple_of(WINDOW + slot * ROWS, ROWS), ROWS)
    for dy in range(4):
        where, _ = target(0, dy)
        ship(
            seg_ref, segb.at[STEPS + (y % 2) * 2 + core], send.at[6], recv.at[6],
            where, stays if dy == 0 else None,
        )
    streams = (
        (k_own, kb, own_rows2, 1, 0, 0),
        (v_own, vb, own_rows2, 1, 0, 1),
        (q_own, qb.at[0], own_rows, 2, 0, 2),
        (q_own, qb.at[1], own_rows, 2, 1, None),
        (g_own, gb.at[0], own_rows, 2, 0, 3),
        (g_own, gb.at[1], own_rows, 2, 1, None),
    )
    for index, (src, dst, rows, per, n, loaded) in enumerate(streams):
        if loaded is not None:
            loads[loaded].wait()
        for dx, dy in offsets:
            where, head = target(dx, dy)
            column = (head * per + n) * HEAD_DIM
            ship(
                src.at[:, pl.ds(pl.multiple_of(column, HEAD_DIM), HEAD_DIM)],
                dst.at[rows, :],
                send.at[index],
                recv.at[index],
                where,
                stays if dx == 0 and dy == 0 else None,
            )

    ring = []
    for index, (buf, here, there) in enumerate(
        (
            (segb, pl.ds(STEPS, STEPS), pl.ds(0, STEPS)),
            (kb, newer, older),
            (vb, newer, older),
        )
    ):
        await_bytes(buf.at[here], recv.at[(6, 0, 1)[index]])
        copy = pltpu.make_async_remote_copy(
            src_ref=buf.at[here], dst_ref=buf.at[there],
            send_sem=ring_send.at[index], recv_sem=ring_recv.at[index],
            device_id=after, device_id_type=MESH,
        )
        pl.when(has_after)(copy.start)
        ring.append(copy)

    kt[:, newer] = kb[newer, :].T
    vt[:, newer] = vb[newer, :].T
    dk_acc[...] = jnp.zeros_like(dk_acc)
    dv_acc[...] = jnp.zeros_like(dv_acc)
    pl.when(has_before)(ring[0].wait_recv)
    rows = [segb[r].astype(jnp.float32) for r in range(2 * STEPS)]
    all_rows = jnp.concatenate(rows, axis=0)
    starts = [
        jnp.sum(
            jnp.sum((all_rows < d).astype(jnp.float32), axis=0, keepdims=True), axis=1, keepdims=True
        )
        for d in range(DOCS)
    ]
    lane = lax.broadcasted_iota(jnp.int32, (1, TILE), 1).astype(jnp.float32)
    for i in range(STEPS):
        row = rows[STEPS + i]
        first = lane + (i * TILE + 1.0)
        for d in range(DOCS):
            first = jnp.maximum(first, jnp.where(row >= d, starts[d], 0.0))
        lo_buf[i] = (first - i * TILE).astype(jnp.int32)
    pl.when(has_before)(ring[1].wait_recv)
    kt[:, older] = kb[older, :].T
    pl.when(has_before)(ring[2].wait_recv)
    vt[:, older] = vb[older, :].T

    key_index = lax.broadcasted_iota(jnp.int32, (SPAN, TILE), 0)
    last_key = WINDOW + lax.broadcasted_iota(jnp.int32, (1, TILE), 1)

    def send_back(buf, out, per, n, i, dx, index):
        yy, c = i // 2, i % 2
        tx = (x + dx) % 4
        ty = core * 2 + yy
        where = ((z * 4 + ty) * 2 + c, tx)
        ship(
            buf.at[pl.ds(pl.multiple_of((i * 4 + tx) * ROWS, ROWS), ROWS), :],
            out.at[:, pl.ds(pl.multiple_of((group * per + n) * HEAD_DIM, HEAD_DIM), HEAD_DIM)],
            out_send.at[index],
            out_recv.at[index],
            where,
            ((ty == y) & (c == core)) if dx == 0 else None,
        )

    def forward(n):
        def step(j, carry):
            for i in (2 * j, 2 * j + 1):
                base = pl.multiple_of(i * TILE, TILE)
                seen = (key_index >= lo_buf[i]) & (key_index <= last_key)
                scores = dot(kb[pl.ds(base, SPAN), :], qb[n, pl.ds(base, TILE), :], ((1,), (1,)))
                scores = jnp.where(seen, scores, HIDDEN)
                top = jnp.max(scores, axis=0, keepdims=True)
                weights = jnp.exp2(scores * EXP2_SCALE - top * EXP2_SCALE)
                total = jnp.sum(weights, axis=0, keepdims=True)
                probs = (weights * (1.0 / total)).astype(jnp.bfloat16)
                pb[n, i] = probs
                out_t = dot(vt[:, pl.ds(base, SPAN)], probs)
                ot[n, i] = out_t
                ab[n, pl.ds(base, TILE), :] = out_t.T.astype(jnp.bfloat16)
            for i in (2 * j, 2 * j + 1):
                for dx in range(4):
                    send_back(ab.at[n], a_ref, 2, n, i, dx, n)
            return carry

        lax.fori_loop(0, STEPS // 2, step, 0)

    def grads_of(n, i):
        base = pl.multiple_of(i * TILE, TILE)
        grads = gb[n, pl.ds(base, TILE), :]
        grads_t = grads.T
        low = ot[n, i].astype(jnp.bfloat16).astype(jnp.float32)
        delta = jnp.sum(low * grads_t.astype(jnp.float32), axis=0, keepdims=True)
        return base, grads, grads_t, delta

    def part(n, i, base, first, count, grads, grads_t, delta):
        span = pl.ds(pl.multiple_of(base + first, TILE), count)
        probs = pb[n, i, first : first + count, :]
        prob_grads = dot(vb[span, :], grads_t)
        score_grads = (probs.astype(jnp.float32) * (prob_grads - delta)).astype(jnp.bfloat16)
        dv_acc[span, :] += dot(probs, grads)
        dk_acc[span, :] += dot(score_grads, qb[n, pl.ds(base, TILE), :])
        return dot(kt[:, span], score_grads)

    def finish(n, i, base, dq_t):
        gqb[n, pl.ds(base, TILE), :] = (dq_t * ATTN_SCALE).T.astype(jnp.bfloat16)

    await_bytes(qb.at[0], recv.at[2])
    forward(0)
    await_bytes(qb.at[1], recv.at[3])
    forward(1)
    await_bytes(gb.at[0], recv.at[4])

    def backward(j, carry):
        for i in (2 * j, 2 * j + 1):
            base, grads, grads_t, delta = grads_of(0, i)
            finish(0, i, base, part(0, i, base, 0, SPAN, grads, grads_t, delta))
        for i in (2 * j, 2 * j + 1):
            for dx in range(4):
                send_back(gqb.at[0], gq_ref, 2, 0, i, dx, 2)
        return carry

    lax.fori_loop(0, STEPS // 2, backward, 0)
    await_bytes(gb.at[1], recv.at[5])

    for i in range(STEPS):
        dq[i] = part(1, i, i * TILE, 0, WINDOW - i * TILE, *grads_of(1, i)[1:])
    dk_out[...] = (dk_acc[older, :] * ATTN_SCALE).astype(jnp.bfloat16)
    dv_out[...] = dv_acc[older, :].astype(jnp.bfloat16)
    back = []
    for index, (src, dst) in enumerate(((dk_out, dk_in), (dv_out, dv_in))):
        copy = pltpu.make_async_remote_copy(
            src_ref=src, dst_ref=dst, send_sem=ring_send.at[3 + index], recv_sem=ring_recv.at[3 + index],
            device_id=before, device_id_type=MESH,
        )
        pl.when(has_before)(copy.start)
        back.append(copy)

    @pl.when(jnp.logical_not(has_after))
    def _():
        dk_in[...] = jnp.zeros_like(dk_in)
        dv_in[...] = jnp.zeros_like(dv_in)

    for i in range(STEPS):
        base, grads, grads_t, delta = grads_of(1, i)
        first = WINDOW - i * TILE
        finish(1, i, base, dq[i] + part(1, i, base, first, SPAN - first, grads, grads_t, delta))
        for dx in range(4):
            send_back(gqb.at[1], gq_ref, 2, 1, i, dx, 3)

    pl.when(has_after)(back[0].wait_recv)
    gkb[...] = (dk_acc[newer, :] * ATTN_SCALE + dk_in[...].astype(jnp.float32)).astype(jnp.bfloat16)
    for i in range(STEPS):
        for dx in range(4):
            send_back(gkb, gk_ref, 1, 0, i, dx, 4)
    pl.when(has_after)(back[1].wait_recv)
    gvb[...] = (dv_acc[newer, :] + dv_in[...].astype(jnp.float32)).astype(jnp.bfloat16)
    for i in range(STEPS):
        for dx in range(4):
            send_back(gvb, gv_ref, 1, 0, i, dx, 5)

    for copy in ring:
        pl.when(has_after)(copy.wait_send)
    for copy in back:
        pl.when(has_before)(copy.wait_send)
    for _ in range(3):
        await_bytes(seg_ref, send.at[6])
    pl.when(leaves)(functools.partial(await_bytes, seg_ref, send.at[6]))
    for sems in (send, out_send):
        for index in range(6):
            await_bytes(gkb.at[pl.ds(0, 15 * ROWS), :], sems.at[index])
            pl.when(leaves)(functools.partial(await_bytes, gkb.at[pl.ds(0, ROWS), :], sems.at[index]))
    everything = pl.ds(0, KVHEADS * HEAD_DIM)
    for index, out in enumerate((a_ref, a_ref, gq_ref, gq_ref, gk_ref, gv_ref)):
        await_bytes(out.at[:, everything], out_recv.at[index])


def deliver(a_ref, gq_ref, gk_ref, gv_ref, *rest):
    outs, sem = rest[:4], rest[4]
    copies = [
        pltpu.make_async_copy(src, dst, sem.at[n])
        for n, (src, dst) in enumerate(zip((a_ref, gq_ref, gk_ref, gv_ref), outs))
    ]
    for copy in copies:
        copy.start()
    for copy in copies:
        copy.wait()


def body(queries, keys, values, grad_out, segments):
    low = jnp.bfloat16
    shape = jax.ShapeDtypeStruct
    outs = (
        shape(queries.shape, low),
        shape(queries.shape, low),
        shape(keys.shape, low),
        shape(keys.shape, low),
    )
    wide, narrow = queries.shape, keys.shape
    queries, keys, values, grad_out, segments = (
        pltpu.with_memory_space_constraint(a, pltpu.HBM)
        for a in (queries, keys, values, grad_out, segments.reshape(1, TILE))
    )
    results = pl.pallas_call(
        kernel,
        out_shape=outs,
        in_specs=[pl.BlockSpec(memory_space=pltpu.HBM)] * 4 + [pl.BlockSpec(memory_space=pltpu.VMEM)],
        out_specs=[pl.BlockSpec(memory_space=pl.ANY)] * 4,
        scratch_shapes=[
            pltpu.VMEM(wide, low),
            pltpu.VMEM(narrow, low),
            pltpu.VMEM(narrow, low),
            pltpu.VMEM(wide, low),
            pltpu.VMEM((2, WINDOW, HEAD_DIM), low),
            pltpu.VMEM((2 * WINDOW, HEAD_DIM), low),
            pltpu.VMEM((2 * WINDOW, HEAD_DIM), low),
            pltpu.VMEM((2, WINDOW, HEAD_DIM), low),
            pltpu.VMEM((2 * STEPS, 1, TILE), jnp.int32),
            pltpu.VMEM((HEAD_DIM, 2 * WINDOW), low),
            pltpu.VMEM((HEAD_DIM, 2 * WINDOW), low),
            pltpu.VMEM((2, STEPS, SPAN, TILE), low),
            pltpu.VMEM((2, STEPS, HEAD_DIM, TILE), jnp.float32),
            pltpu.VMEM((STEPS, HEAD_DIM, TILE), jnp.float32),
            pltpu.VMEM((STEPS, 1, TILE), jnp.int32),
            pltpu.VMEM((2, WINDOW, HEAD_DIM), low),
            pltpu.VMEM((2, WINDOW, HEAD_DIM), low),
            pltpu.VMEM((2 * WINDOW, HEAD_DIM), jnp.float32),
            pltpu.VMEM((2 * WINDOW, HEAD_DIM), jnp.float32),
            pltpu.VMEM((WINDOW, HEAD_DIM), low),
            pltpu.VMEM((WINDOW, HEAD_DIM), low),
            pltpu.VMEM((WINDOW, HEAD_DIM), low),
            pltpu.VMEM((WINDOW, HEAD_DIM), low),
            pltpu.VMEM((WINDOW, HEAD_DIM), low),
            pltpu.VMEM((WINDOW, HEAD_DIM), low),
            pltpu.SemaphoreType.DMA((4,)),
            pltpu.SemaphoreType.DMA((7,)),
            pltpu.SemaphoreType.DMA((7,)),
            pltpu.SemaphoreType.DMA((5,)),
            pltpu.SemaphoreType.DMA((5,)),
            pltpu.SemaphoreType.DMA((6,)),
            pltpu.SemaphoreType.DMA((6,)),
        ],
        compiler_params=pltpu.CompilerParams(
            collective_id=0, has_side_effects=True, vmem_limit_bytes=48 * 1024 * 1024
        ),
    )(queries, keys, values, grad_out, segments)
    return pl.pallas_call(
        deliver,
        out_shape=outs,
        in_specs=[pl.BlockSpec(memory_space=pltpu.VMEM)] * 4,
        out_specs=[pl.BlockSpec(memory_space=pl.ANY)] * 4,
        scratch_shapes=[pltpu.SemaphoreType.DMA((4,))],
        compiler_params=pltpu.CompilerParams(vmem_limit_bytes=8 * 1024 * 1024),
    )(*results)


def solution(mesh):
    spec = P(("ctx", "head"), None)
    return jax.shard_map(
        body,
        mesh=mesh,
        in_specs=(spec, spec, spec, spec, P("ctx")),
        out_specs=(spec, spec, spec, spec),
        check_vma=False,
    )
```

```python
import functools
import math

import jax
import jax.numpy as jnp
from jax import lax
from jax.experimental import pallas as pl
from jax.experimental.pallas import tpu as pltpu
from jax.sharding import PartitionSpec as P

QHEADS = 32
KVHEADS = 16
HEAD_DIM = 128
WINDOW = 1024
DOCS = 8

ATTN_SCALE = 168.0 ** (-0.5)
EXP2_SCALE = ATTN_SCALE * math.log2(math.e)
MESH = pl.DeviceIdType.MESH

ROWS = 64
TILE = 256
STEPS = WINDOW // TILE
SPAN = WINDOW + TILE
HIDDEN = -1e30
APART = 2.0**17
WIDE = 2 * HEAD_DIM


def dot(a, b, dims=((1,), (0,))):
    return lax.dot_general(a, b, (dims, ((), ())), preferred_element_type=jnp.float32)


def await_bytes(ref, sem):
    pltpu.make_async_copy(ref, ref, sem).wait()


def kernel(
    q_ref, k_ref, v_ref, g_ref, seg_ref,
    a_ref, gq_ref, gk_ref, gv_ref,
    q_own, k_own, v_own, g_own,
    qb, kb, vb, gb, segb,
    kt, vt, sb, pb, ot, inv, dq, ab, gqb, dk_acc, dv_acc, dk_out, dv_out, dk_in, dv_in, gkb, gvb,
    load, send, recv, ring_send, ring_recv, out_send, out_recv,
):
    ctx, x = lax.axis_index("ctx"), lax.axis_index("head")
    core, y, z = ctx % 2, (ctx // 2) % 4, ctx // 8
    planes = lax.axis_size("ctx") // 8
    half = y // 2
    slot = ((y % 2) * 2 + core) * 4 + x
    group = x * 4 + y
    has_after = (z < planes - 1) | (core == 0)
    has_before = (z > 0) | (core == 1)
    after = (jnp.where(core == 0, ctx + 1, ((z + 1) % planes) * 8 + y * 2), x)
    before = (jnp.where(core == 1, ctx - 1, ((z + planes - 1) % planes) * 8 + y * 2 + 1), x)
    stays = half == core
    leaves = jnp.logical_not(stays)

    def source(yy, c, dx):
        return ((z * 4 + core * 2 + yy) * 2 + c, (x + dx) % 4)

    barrier = pltpu.get_barrier_semaphore()
    for yy in range(2):
        for c in range(2):
            for dx in range(4):
                pl.semaphore_signal(barrier, inc=1, device_id=source(yy, c, dx), device_id_type=MESH)

    @pl.when(has_before)
    def _():
        pl.semaphore_signal(barrier, inc=1, device_id=before, device_id_type=MESH)

    loads = [
        pltpu.make_async_copy(src, dst, load.at[n])
        for n, (src, dst) in enumerate(
            ((k_ref, k_own), (v_ref, v_own), (q_ref, q_own), (g_ref, g_own))
        )
    ]
    for copy in loads:
        copy.start()
    newer, older = pl.ds(WINDOW, WINDOW), pl.ds(0, WINDOW)

    @pl.when(jnp.logical_not(has_before))
    def _():
        kb[older, slice(0, HEAD_DIM)] = jnp.zeros((WINDOW, HEAD_DIM), kb.dtype)
        vb[older, :] = jnp.zeros((WINDOW, HEAD_DIM), vb.dtype)
        segb[pl.ds(0, STEPS)] = jnp.full((STEPS, 1, TILE), -1, segb.dtype)

    pl.semaphore_wait(barrier, 16 + has_after.astype(jnp.int32))

    def target(dx, dy):
        tx, ty = (x + dx) % 4, (y + dy) % 4
        return ((z * 4 + ty) * 2 + half, tx), tx * 4 + ty

    def ship(src, dst, send_sem, recv_sem, where, local):
        def far():
            pltpu.make_async_remote_copy(
                src_ref=src, dst_ref=dst, send_sem=send_sem, recv_sem=recv_sem,
                device_id=where, device_id_type=MESH,
            ).start()

        if local is None:
            far()
        else:
            pl.when(local)(lambda: pltpu.make_async_copy(src, dst, recv_sem).start())
            pl.when(jnp.logical_not(local))(far)

    offsets = [(dx, dy) for dx in range(4) for dy in range(4)]
    offsets = sorted(offsets, key=lambda o: -min(o[0], 4 - o[0]) - min(o[1], 4 - o[1]))
    own_rows = pl.ds(pl.multiple_of(slot * ROWS, ROWS), ROWS)
    own_rows2 = pl.ds(pl.multiple_of(WINDOW + slot * ROWS, ROWS), ROWS)
    for dy in range(4):
        where, _ = target(0, dy)
        ship(
            seg_ref, segb.at[STEPS + (y % 2) * 2 + core], send.at[6], recv.at[6],
            where, stays if dy == 0 else None,
        )
    head_part, doc_part = pl.ds(0, HEAD_DIM), pl.ds(HEAD_DIM, HEAD_DIM)
    streams = (
        (k_own, kb.at[:, head_part], own_rows2, 1, 0, 0),
        (v_own, vb, own_rows2, 1, 0, 1),
        (q_own, qb.at[0, :, head_part], own_rows, 2, 0, 2),
        (q_own, qb.at[1, :, head_part], own_rows, 2, 1, None),
        (g_own, gb.at[0], own_rows, 2, 0, 3),
        (g_own, gb.at[1], own_rows, 2, 1, None),
    )
    for index, (src, dst, rows, per, n, loaded) in enumerate(streams):
        if loaded is not None:
            loads[loaded].wait()
        for dx, dy in offsets:
            where, head = target(dx, dy)
            column = (head * per + n) * HEAD_DIM
            ship(
                src.at[:, pl.ds(pl.multiple_of(column, HEAD_DIM), HEAD_DIM)],
                dst.at[rows, :],
                send.at[index],
                recv.at[index],
                where,
                stays if dx == 0 and dy == 0 else None,
            )

    ring = []
    for index, (buf, here, there) in enumerate(
        (
            (segb, pl.ds(STEPS, STEPS), pl.ds(0, STEPS)),
            (kb.at[:, head_part], newer, older),
            (vb, newer, older),
        )
    ):
        await_bytes(buf.at[here], recv.at[(6, 0, 1)[index]])
        copy = pltpu.make_async_remote_copy(
            src_ref=buf.at[here], dst_ref=buf.at[there],
            send_sem=ring_send.at[index], recv_sem=ring_recv.at[index],
            device_id=after, device_id_type=MESH,
        )
        pl.when(has_after)(copy.start)
        ring.append(copy)

    kind = lax.broadcasted_iota(jnp.int32, (HEAD_DIM, TILE), 0)

    def documents(r):
        number = segb[r]
        number = jnp.where(number < 0, DOCS, number)
        return jnp.where(kind == number, 1.0, 0.0).T

    for r in range(STEPS):
        hot = documents(STEPS + r)
        kb[pl.ds(WINDOW + r * TILE, TILE), doc_part] = hot.astype(kb.dtype)
        apart = ((hot - 1.0) * APART).astype(qb.dtype)
        for n in range(2):
            qb[n, pl.ds(r * TILE, TILE), doc_part] = apart
    kt[:, newer] = kb[newer, head_part].T
    vt[:, newer] = vb[newer, :].T
    dk_acc[...] = jnp.zeros_like(dk_acc)
    dv_acc[...] = jnp.zeros_like(dv_acc)
    pl.when(has_before)(ring[0].wait_recv)
    for r in range(STEPS):
        kb[pl.ds(r * TILE, TILE), doc_part] = documents(r).astype(kb.dtype)
    pl.when(has_before)(ring[1].wait_recv)
    kt[:, older] = kb[older, head_part].T
    pl.when(has_before)(ring[2].wait_recv)
    vt[:, older] = vb[older, :].T

    key_at = lax.broadcasted_iota(jnp.int32, (TILE, TILE), 0)
    query_at = lax.broadcasted_iota(jnp.int32, (TILE, TILE), 1)

    def send_back(buf, out, per, n, index):
        column = pl.ds(pl.multiple_of((group * per + n) * HEAD_DIM, HEAD_DIM), HEAD_DIM)
        for dx in (2, 1, 3, 0):
            for turn in range(2):
                for c in range(2):
                    yy = (y + turn) % 2
                    tx, ty = (x + dx) % 4, core * 2 + yy
                    ship(
                        buf.at[pl.ds(pl.multiple_of(((yy * 2 + c) * 4 + tx) * ROWS, ROWS), ROWS), :],
                        out.at[:, column],
                        out_send.at[index],
                        out_recv.at[index],
                        ((z * 4 + ty) * 2 + c, tx),
                        ((ty == y) & (c == core)) if dx == 0 and turn == 0 else None,
                    )

    def forward(n):
        def score(i, t):
            rows = pl.ds(t * TILE, TILE)
            scores = dot(
                kb[pl.ds((i + t) * TILE, TILE), :], qb[n, pl.ds(i * TILE, TILE), :], ((1,), (1,))
            )
            if t == 0:
                scores = jnp.where(key_at > query_at, scores, HIDDEN)
            if t == STEPS:
                scores = jnp.where(key_at <= query_at, scores, HIDDEN)
            sb[i % 2, rows, :] = scores
            return jnp.max(scores, axis=0, keepdims=True)

        tops = [score(0, t) for t in range(STEPS + 1)]
        for i in range(STEPS):
            top, tops, total = functools.reduce(jnp.maximum, tops), [], 0.0
            for t in range(STEPS + 1):
                rows = pl.ds(t * TILE, TILE)
                weights = jnp.exp2((sb[i % 2, rows, :] - top) * EXP2_SCALE)
                total = total + jnp.sum(weights, axis=0, keepdims=True)
                pb[n, i, rows, :] = weights.astype(jnp.bfloat16)
                if i + 1 < STEPS:
                    tops.append(score(i + 1, t))
            scale = 1.0 / total
            inv[n, i] = scale
            out_t = (dot(vt[:, pl.ds(i * TILE, SPAN)], pb[n, i]) * scale).astype(jnp.bfloat16)
            ot[n, i] = out_t
            ab[n, pl.ds(i * TILE, TILE), :] = out_t.T
        send_back(ab.at[n], a_ref, 2, n, n)

    def grads_of(n, i):
        base = pl.multiple_of(i * TILE, TILE)
        grads_t = gb[n, pl.ds(base, TILE), :].T.astype(jnp.float32) * inv[n, i]
        grads_t = grads_t.astype(jnp.bfloat16)
        delta = jnp.sum(
            ot[n, i].astype(jnp.float32) * grads_t.astype(jnp.float32), axis=0, keepdims=True
        )
        return base, grads_t, delta

    def part(n, i, base, first, count, grads_t, delta):
        span = pl.ds(pl.multiple_of(base + first, TILE), count)
        weights = pb[n, i, first : first + count, :]
        prob_grads = dot(vb[span, :], grads_t)
        score_grads = (weights.astype(jnp.float32) * (prob_grads - delta)).astype(jnp.bfloat16)
        dv_acc[span, :] += dot(weights, grads_t, ((1,), (1,)))
        dk_acc[span, :] += dot(score_grads, qb[n, pl.ds(base, TILE), head_part])
        return dot(kt[:, span], score_grads)

    def finish(n, i, base, dq_t):
        gqb[n, pl.ds(base, TILE), :] = (dq_t * ATTN_SCALE).T.astype(jnp.bfloat16)

    await_bytes(qb.at[0, :, head_part], recv.at[2])
    forward(0)
    await_bytes(qb.at[1, :, head_part], recv.at[3])
    forward(1)
    await_bytes(gb.at[0], recv.at[4])

    def backward(j, carry):
        for i in (2 * j, 2 * j + 1):
            base, grads_t, delta = grads_of(0, i)
            finish(0, i, base, part(0, i, base, 0, SPAN, grads_t, delta))
        return carry

    lax.fori_loop(0, STEPS // 2, backward, 0)
    send_back(gqb.at[0], gq_ref, 2, 0, 2)
    await_bytes(gb.at[1], recv.at[5])

    for i in range(STEPS):
        dq[i] = part(1, i, i * TILE, 0, WINDOW - i * TILE, *grads_of(1, i)[1:])
    dk_out[...] = (dk_acc[older, :] * ATTN_SCALE).astype(jnp.bfloat16)
    dv_out[...] = dv_acc[older, :].astype(jnp.bfloat16)
    back = []
    for index, (src, dst) in enumerate(((dk_out, dk_in), (dv_out, dv_in))):
        copy = pltpu.make_async_remote_copy(
            src_ref=src, dst_ref=dst, send_sem=ring_send.at[3 + index], recv_sem=ring_recv.at[3 + index],
            device_id=before, device_id_type=MESH,
        )
        pl.when(has_before)(copy.start)
        back.append(copy)

    @pl.when(jnp.logical_not(has_after))
    def _():
        dk_in[...] = jnp.zeros_like(dk_in)
        dv_in[...] = jnp.zeros_like(dv_in)

    for i in range(STEPS):
        base, grads_t, delta = grads_of(1, i)
        first = WINDOW - i * TILE
        finish(1, i, base, dq[i] + part(1, i, base, first, SPAN - first, grads_t, delta))
    send_back(gqb.at[1], gq_ref, 2, 1, 3)

    pl.when(has_after)(back[0].wait_recv)
    gkb[...] = (dk_acc[newer, :] * ATTN_SCALE + dk_in[...].astype(jnp.float32)).astype(jnp.bfloat16)
    send_back(gkb, gk_ref, 1, 0, 4)
    pl.when(has_after)(back[1].wait_recv)
    gvb[...] = (dv_acc[newer, :] + dv_in[...].astype(jnp.float32)).astype(jnp.bfloat16)
    send_back(gvb, gv_ref, 1, 0, 5)

    for copy in ring:
        pl.when(has_after)(copy.wait_send)
    for copy in back:
        pl.when(has_before)(copy.wait_send)
    for _ in range(3):
        await_bytes(seg_ref, send.at[6])
    pl.when(leaves)(functools.partial(await_bytes, seg_ref, send.at[6]))
    for sems in (send, out_send):
        for index in range(6):
            await_bytes(gkb.at[pl.ds(0, 15 * ROWS), :], sems.at[index])
            pl.when(leaves)(functools.partial(await_bytes, gkb.at[pl.ds(0, ROWS), :], sems.at[index]))
    everything = pl.ds(0, KVHEADS * HEAD_DIM)
    for index, out in enumerate((a_ref, a_ref, gq_ref, gq_ref, gk_ref, gv_ref)):
        await_bytes(out.at[:, everything], out_recv.at[index])


def deliver(a_ref, gq_ref, gk_ref, gv_ref, *rest):
    outs, sem = rest[:4], rest[4]
    copies = [
        pltpu.make_async_copy(src, dst, sem.at[n])
        for n, (src, dst) in enumerate(zip((a_ref, gq_ref, gk_ref, gv_ref), outs))
    ]
    for copy in copies:
        copy.start()
    for copy in copies:
        copy.wait()


def body(queries, keys, values, grad_out, segments):
    low = jnp.bfloat16
    shape = jax.ShapeDtypeStruct
    outs = (
        shape(queries.shape, low),
        shape(queries.shape, low),
        shape(keys.shape, low),
        shape(keys.shape, low),
    )
    wide, narrow = queries.shape, keys.shape
    queries, keys, values, grad_out, segments = (
        pltpu.with_memory_space_constraint(a, pltpu.HBM)
        for a in (queries, keys, values, grad_out, segments.reshape(1, TILE))
    )
    results = pl.pallas_call(
        kernel,
        out_shape=outs,
        in_specs=[pl.BlockSpec(memory_space=pltpu.HBM)] * 4 + [pl.BlockSpec(memory_space=pltpu.VMEM)],
        out_specs=[pl.BlockSpec(memory_space=pl.ANY)] * 4,
        scratch_shapes=[
            pltpu.VMEM(wide, low),
            pltpu.VMEM(narrow, low),
            pltpu.VMEM(narrow, low),
            pltpu.VMEM(wide, low),
            pltpu.VMEM((2, WINDOW, WIDE), low),
            pltpu.VMEM((2 * WINDOW, WIDE), low),
            pltpu.VMEM((2 * WINDOW, HEAD_DIM), low),
            pltpu.VMEM((2, WINDOW, HEAD_DIM), low),
            pltpu.VMEM((2 * STEPS, 1, TILE), jnp.int32),
            pltpu.VMEM((HEAD_DIM, 2 * WINDOW), low),
            pltpu.VMEM((HEAD_DIM, 2 * WINDOW), low),
            pltpu.VMEM((2, SPAN, TILE), jnp.float32),
            pltpu.VMEM((2, STEPS, SPAN, TILE), low),
            pltpu.VMEM((2, STEPS, HEAD_DIM, TILE), low),
            pltpu.VMEM((2, STEPS, 1, TILE), jnp.float32),
            pltpu.VMEM((STEPS, HEAD_DIM, TILE), jnp.float32),
            pltpu.VMEM((2, WINDOW, HEAD_DIM), low),
            pltpu.VMEM((2, WINDOW, HEAD_DIM), low),
            pltpu.VMEM((2 * WINDOW, HEAD_DIM), jnp.float32),
            pltpu.VMEM((2 * WINDOW, HEAD_DIM), jnp.float32),
            pltpu.VMEM((WINDOW, HEAD_DIM), low),
            pltpu.VMEM((WINDOW, HEAD_DIM), low),
            pltpu.VMEM((WINDOW, HEAD_DIM), low),
            pltpu.VMEM((WINDOW, HEAD_DIM), low),
            pltpu.VMEM((WINDOW, HEAD_DIM), low),
            pltpu.VMEM((WINDOW, HEAD_DIM), low),
            pltpu.SemaphoreType.DMA((4,)),
            pltpu.SemaphoreType.DMA((7,)),
            pltpu.SemaphoreType.DMA((7,)),
            pltpu.SemaphoreType.DMA((5,)),
            pltpu.SemaphoreType.DMA((5,)),
            pltpu.SemaphoreType.DMA((6,)),
            pltpu.SemaphoreType.DMA((6,)),
        ],
        compiler_params=pltpu.CompilerParams(
            collective_id=0, has_side_effects=True, vmem_limit_bytes=48 * 1024 * 1024
        ),
    )(queries, keys, values, grad_out, segments)
    return pl.pallas_call(
        deliver,
        out_shape=outs,
        in_specs=[pl.BlockSpec(memory_space=pltpu.VMEM)] * 4,
        out_specs=[pl.BlockSpec(memory_space=pl.ANY)] * 4,
        scratch_shapes=[pltpu.SemaphoreType.DMA((4,))],
        compiler_params=pltpu.CompilerParams(vmem_limit_bytes=8 * 1024 * 1024),
    )(*results)


def solution(mesh):
    spec = P(("ctx", "head"), None)
    return jax.shard_map(
        body,
        mesh=mesh,
        in_specs=(spec, spec, spec, spec, P("ctx")),
        out_specs=(spec, spec, spec, spec),
        check_vma=False,
    )
```

```python
import functools
import math

import jax
import jax.numpy as jnp
from jax import lax
from jax.experimental import pallas as pl
from jax.experimental.pallas import tpu as pltpu
from jax.sharding import PartitionSpec as P

QHEADS = 32
KVHEADS = 16
HEAD_DIM = 128
WINDOW = 1024
DOCS = 8

ATTN_SCALE = 168.0 ** (-0.5)
EXP2_SCALE = ATTN_SCALE * math.log2(math.e)
MESH = pl.DeviceIdType.MESH

ROWS = 64
TILE = 256
STEPS = WINDOW // TILE
SPAN = WINDOW + TILE
HIDDEN = -1e30
APART = 2.0**17
WIDE = 2 * HEAD_DIM


def dot(a, b, dims=((1,), (0,))):
    return lax.dot_general(a, b, (dims, ((), ())), preferred_element_type=jnp.float32)


def await_bytes(ref, sem):
    pltpu.make_async_copy(ref, ref, sem).wait()


def kernel(
    q_ref, k_ref, v_ref, g_ref, seg_ref,
    a_ref, gq_ref, gk_ref, gv_ref,
    q_own, k_own, v_own, g_own, seg_own,
    qb, kb, vb, gb, segb,
    kt, vt, sb, pb, ot, inv, dq, ab, gqb, dk_acc, dv_acc, dk_out, dv_out, dk_in, dv_in, gkb, gvb,
    load, send, recv, ring_send, ring_recv, out_send, out_recv,
):
    ctx, x = lax.axis_index("ctx"), lax.axis_index("head")
    core, y, z = ctx % 2, (ctx // 2) % 4, ctx // 8
    planes = lax.axis_size("ctx") // 8
    half = y // 2
    slot = ((y % 2) * 2 + core) * 4 + x
    group = x * 4 + y
    has_after = (z < planes - 1) | (core == 0)
    has_before = (z > 0) | (core == 1)
    after = (jnp.where(core == 0, ctx + 1, ((z + 1) % planes) * 8 + y * 2), x)
    before = (jnp.where(core == 1, ctx - 1, ((z + planes - 1) % planes) * 8 + y * 2 + 1), x)
    stays = half == core
    leaves = jnp.logical_not(stays)

    def source(yy, c, dx):
        return ((z * 4 + core * 2 + yy) * 2 + c, (x + dx) % 4)

    barrier = pltpu.get_barrier_semaphore()
    for yy in range(2):
        for c in range(2):
            for dx in range(4):
                pl.semaphore_signal(barrier, inc=1, device_id=source(yy, c, dx), device_id_type=MESH)

    @pl.when(has_before)
    def _():
        pl.semaphore_signal(barrier, inc=1, device_id=before, device_id_type=MESH)

    loads = [
        pltpu.make_async_copy(src, dst, load.at[n])
        for n, (src, dst) in enumerate(
            (
                (k_ref, k_own),
                (v_ref, v_own),
                (q_ref, q_own),
                (g_ref, g_own),
                (seg_ref, seg_own),
            )
        )
    ]
    for copy in loads:
        copy.start()
    newer, older = pl.ds(WINDOW, WINDOW), pl.ds(0, WINDOW)

    @pl.when(jnp.logical_not(has_before))
    def _():
        kb[older, slice(0, HEAD_DIM)] = jnp.zeros((WINDOW, HEAD_DIM), kb.dtype)
        vb[older, :] = jnp.zeros((WINDOW, HEAD_DIM), vb.dtype)
        segb[pl.ds(0, STEPS)] = jnp.full((STEPS, 1, TILE), -1, segb.dtype)

    pl.semaphore_wait(barrier, 16 + has_after.astype(jnp.int32))

    def target(dx, dy):
        tx, ty = (x + dx) % 4, (y + dy) % 4
        return ((z * 4 + ty) * 2 + half, tx), tx * 4 + ty

    def ship(src, dst, send_sem, recv_sem, where, local):
        def far():
            pltpu.make_async_remote_copy(
                src_ref=src, dst_ref=dst, send_sem=send_sem, recv_sem=recv_sem,
                device_id=where, device_id_type=MESH,
            ).start()

        if local is None:
            far()
        else:
            pl.when(local)(lambda: pltpu.make_async_copy(src, dst, recv_sem).start())
            pl.when(jnp.logical_not(local))(far)

    offsets = [(dx, dy) for dx in range(4) for dy in range(4)]
    offsets = sorted(offsets, key=lambda o: -min(o[0], 4 - o[0]) - min(o[1], 4 - o[1]))
    own_rows = pl.ds(pl.multiple_of(slot * ROWS, ROWS), ROWS)
    own_rows2 = pl.ds(pl.multiple_of(WINDOW + slot * ROWS, ROWS), ROWS)
    loads[4].wait()
    for dy in range(4):
        where, _ = target(0, dy)
        ship(
            seg_own, segb.at[STEPS + (y % 2) * 2 + core], send.at[6], recv.at[6],
            where, stays if dy == 0 else None,
        )
    head_part, doc_part = pl.ds(0, HEAD_DIM), pl.ds(HEAD_DIM, HEAD_DIM)
    streams = (
        (k_own, kb.at[:, head_part], own_rows2, 1, 0, 0),
        (v_own, vb, own_rows2, 1, 0, 1),
        (q_own, qb.at[0, :, head_part], own_rows, 2, 0, 2),
        (q_own, qb.at[1, :, head_part], own_rows, 2, 1, None),
        (g_own, gb.at[0], own_rows, 2, 0, 3),
        (g_own, gb.at[1], own_rows, 2, 1, None),
    )
    for index, (src, dst, rows, per, n, loaded) in enumerate(streams):
        if loaded is not None:
            loads[loaded].wait()
        for dx, dy in offsets:
            where, head = target(dx, dy)
            column = (head * per + n) * HEAD_DIM
            ship(
                src.at[:, pl.ds(pl.multiple_of(column, HEAD_DIM), HEAD_DIM)],
                dst.at[rows, :],
                send.at[index],
                recv.at[index],
                where,
                stays if dx == 0 and dy == 0 else None,
            )

    ring = []
    for index, (buf, here, there) in enumerate(
        (
            (segb, pl.ds(STEPS, STEPS), pl.ds(0, STEPS)),
            (kb.at[:, head_part], newer, older),
            (vb, newer, older),
        )
    ):
        await_bytes(buf.at[here], recv.at[(6, 0, 1)[index]])
        copy = pltpu.make_async_remote_copy(
            src_ref=buf.at[here], dst_ref=buf.at[there],
            send_sem=ring_send.at[index], recv_sem=ring_recv.at[index],
            device_id=after, device_id_type=MESH,
        )
        pl.when(has_after)(copy.start)
        ring.append(copy)

    kind = lax.broadcasted_iota(jnp.int32, (HEAD_DIM, TILE), 0)

    def documents(r):
        number = segb[r]
        number = jnp.where(number < 0, DOCS, number)
        return jnp.where(kind == number, 1.0, 0.0).T

    for r in range(STEPS):
        hot = documents(STEPS + r)
        kb[pl.ds(WINDOW + r * TILE, TILE), doc_part] = hot.astype(kb.dtype)
        apart = ((hot - 1.0) * APART).astype(qb.dtype)
        for n in range(2):
            qb[n, pl.ds(r * TILE, TILE), doc_part] = apart
    kt[:, newer] = kb[newer, head_part].T
    vt[:, newer] = vb[newer, :].T
    dk_acc[...] = jnp.zeros_like(dk_acc)
    dv_acc[...] = jnp.zeros_like(dv_acc)
    pl.when(has_before)(ring[0].wait_recv)
    for r in range(STEPS):
        kb[pl.ds(r * TILE, TILE), doc_part] = documents(r).astype(kb.dtype)
    pl.when(has_before)(ring[1].wait_recv)
    kt[:, older] = kb[older, head_part].T

    key_at = lax.broadcasted_iota(jnp.int32, (TILE, TILE), 0)
    query_at = lax.broadcasted_iota(jnp.int32, (TILE, TILE), 1)

    def send_block(buf, out, per, n, index, yy, c, dx, maybe_here):
        tx, ty = (x + dx) % 4, core * 2 + yy
        ship(
            buf.at[pl.ds(pl.multiple_of(((yy * 2 + c) * 4 + tx) * ROWS, ROWS), ROWS), :],
            out.at[:, pl.ds(pl.multiple_of((group * per + n) * HEAD_DIM, HEAD_DIM), HEAD_DIM)],
            out_send.at[index],
            out_recv.at[index],
            ((z * 4 + ty) * 2 + c, tx),
            ((ty == y) & (c == core)) if maybe_here else None,
        )

    def send_back(buf, out, per, n, index):
        for dx in (2, 1, 3, 0):
            for turn in range(2):
                for c in range(2):
                    here = dx == 0 and turn == 0
                    send_block(buf, out, per, n, index, (y + turn) % 2, c, dx, here)

    def forward(n):
        def score(i, t):
            rows = pl.ds(t * TILE, TILE)
            scores = dot(
                kb[pl.ds((i + t) * TILE, TILE), :], qb[n, pl.ds(i * TILE, TILE), :], ((1,), (1,))
            )
            if t == 0:
                scores = jnp.where(key_at > query_at, scores, HIDDEN)
            if t == STEPS:
                scores = jnp.where(key_at <= query_at, scores, HIDDEN)
            sb[i % 2, rows, :] = scores
            return jnp.max(scores, axis=0, keepdims=True)

        tops = [score(0, t) for t in range(STEPS + 1)]
        for i in range(STEPS):
            top, tops, total = functools.reduce(jnp.maximum, tops), [], 0.0
            for t in range(STEPS + 1):
                rows = pl.ds(t * TILE, TILE)
                weights = jnp.exp2((sb[i % 2, rows, :] - top) * EXP2_SCALE)
                total = total + jnp.sum(weights, axis=0, keepdims=True)
                pb[n, i, rows, :] = weights.astype(jnp.bfloat16)
                if i + 1 < STEPS:
                    tops.append(score(i + 1, t))
            scale = 1.0 / total
            inv[n, i] = scale
            if n == 0 and i == 0:
                pl.when(has_before)(ring[2].wait_recv)
                vt[:, older] = vb[older, :].T
            out_t = (dot(vt[:, pl.ds(i * TILE, SPAN)], pb[n, i]) * scale).astype(jnp.bfloat16)
            ot[n, i] = out_t
            ab[n, pl.ds(i * TILE, TILE), :] = out_t.T
        send_back(ab.at[n], a_ref, 2, n, n)

    def grads_of(n, i):
        base = pl.multiple_of(i * TILE, TILE)
        grads_t = gb[n, pl.ds(base, TILE), :].T.astype(jnp.float32) * inv[n, i]
        grads_t = grads_t.astype(jnp.bfloat16)
        delta = jnp.sum(
            ot[n, i].astype(jnp.float32) * grads_t.astype(jnp.float32), axis=0, keepdims=True
        )
        return base, grads_t, delta

    def part(n, i, base, first, count, grads_t, delta):
        span = pl.ds(pl.multiple_of(base + first, TILE), count)
        weights = pb[n, i, first : first + count, :]
        prob_grads = dot(vb[span, :], grads_t)
        score_grads = (weights.astype(jnp.float32) * (prob_grads - delta)).astype(jnp.bfloat16)
        dv_acc[span, :] += dot(weights, grads_t, ((1,), (1,)))
        dk_acc[span, :] += dot(score_grads, qb[n, pl.ds(base, TILE), head_part])
        return dot(kt[:, span], score_grads)

    def finish(n, i, base, dq_t):
        gqb[n, pl.ds(base, TILE), :] = (dq_t * ATTN_SCALE).T.astype(jnp.bfloat16)

    await_bytes(qb.at[0, :, head_part], recv.at[2])
    forward(0)
    await_bytes(qb.at[1, :, head_part], recv.at[3])
    forward(1)
    await_bytes(gb.at[0], recv.at[4])

    def backward(j, carry):
        for i in (2 * j, 2 * j + 1):
            base, grads_t, delta = grads_of(0, i)
            finish(0, i, base, part(0, i, base, 0, SPAN, grads_t, delta))
        return carry

    lax.fori_loop(0, STEPS // 2, backward, 0)
    send_back(gqb.at[0], gq_ref, 2, 0, 2)
    await_bytes(gb.at[1], recv.at[5])

    def returned(b, index, src, dst):
        rows = pl.ds(pl.multiple_of(b * TILE, TILE), TILE)
        return pltpu.make_async_remote_copy(
            src_ref=src.at[rows, :], dst_ref=dst.at[rows, :],
            send_sem=ring_send.at[3 + index * STEPS + b], recv_sem=ring_recv.at[3 + index * STEPS + b],
            device_id=before, device_id_type=MESH,
        )

    for i in range(STEPS):
        dq[i] = part(1, i, i * TILE, 0, WINDOW - i * TILE, *grads_of(1, i)[1:])
        rows = pl.ds(i * TILE, TILE)
        dk_out[rows, :] = (dk_acc[rows, :] * ATTN_SCALE).astype(jnp.bfloat16)
        dv_out[rows, :] = dv_acc[rows, :].astype(jnp.bfloat16)

        @pl.when(has_before)
        def _():
            returned(i, 0, dk_out, dk_in).start()
            returned(i, 1, dv_out, dv_in).start()

    @pl.when(jnp.logical_not(has_after))
    def _():
        dk_in[...] = jnp.zeros_like(dk_in)
        dv_in[...] = jnp.zeros_like(dv_in)

    for i in range(STEPS):
        base, grads_t, delta = grads_of(1, i)
        first = WINDOW - i * TILE
        finish(1, i, base, dq[i] + part(1, i, base, first, SPAN - first, grads_t, delta))
    send_back(gqb.at[1], gq_ref, 2, 1, 3)

    first_block = 0 * y

    def settle(step, carry):
        b = (step + first_block) % STEPS
        rows = pl.ds(pl.multiple_of(b * TILE, TILE), TILE)
        rows_acc = pl.ds(pl.multiple_of(WINDOW + b * TILE, TILE), TILE)
        for index, (acc, factor, src, came, buf, out) in enumerate(
            (
                (dk_acc, ATTN_SCALE, dk_out, dk_in, gkb, gk_ref),
                (dv_acc, 1.0, dv_out, dv_in, gvb, gv_ref),
            )
        ):
            pl.when(has_after)(returned(b, index, src, came).wait_recv)
            total = acc[rows_acc, :] * factor + came[rows, :].astype(jnp.float32)
            buf[rows, :] = total.astype(jnp.bfloat16)
            for dx in (2, 1, 3, 0):
                send_block(buf, out, 1, 0, 4 + index, b // 2, b % 2, dx, dx == 0)
        return carry

    lax.fori_loop(0, STEPS, settle, 0)

    for copy in ring:
        pl.when(has_after)(copy.wait_send)

    @pl.when(has_before)
    def _():
        for b in range(STEPS):
            returned(b, 0, dk_out, dk_in).wait_send()
            returned(b, 1, dv_out, dv_in).wait_send()

    for _ in range(3):
        await_bytes(seg_own, send.at[6])
    pl.when(leaves)(functools.partial(await_bytes, seg_own, send.at[6]))
    for sems in (send, out_send):
        for index in range(6):
            await_bytes(gkb.at[pl.ds(0, 15 * ROWS), :], sems.at[index])
            pl.when(leaves)(functools.partial(await_bytes, gkb.at[pl.ds(0, ROWS), :], sems.at[index]))
    everything = pl.ds(0, KVHEADS * HEAD_DIM)
    for index, out in enumerate((a_ref, a_ref, gq_ref, gq_ref, gk_ref, gv_ref)):
        await_bytes(out.at[:, everything], out_recv.at[index])


def deliver(a_ref, gq_ref, gk_ref, gv_ref, *rest):
    outs, sem = rest[:4], rest[4]
    copies = [
        pltpu.make_async_copy(src, dst, sem.at[n])
        for n, (src, dst) in enumerate(zip((a_ref, gq_ref, gk_ref, gv_ref), outs))
    ]
    for copy in copies:
        copy.start()
    for copy in copies:
        copy.wait()


def body(queries, keys, values, grad_out, segments):
    low = jnp.bfloat16
    shape = jax.ShapeDtypeStruct
    outs = (
        shape(queries.shape, low),
        shape(queries.shape, low),
        shape(keys.shape, low),
        shape(keys.shape, low),
    )
    wide, narrow = queries.shape, keys.shape
    queries, keys, values, grad_out, segments = (
        pltpu.with_memory_space_constraint(a, pltpu.HBM)
        for a in (queries, keys, values, grad_out, segments.reshape(1, TILE))
    )
    results = pl.pallas_call(
        kernel,
        out_shape=outs,
        in_specs=[pl.BlockSpec(memory_space=pltpu.HBM)] * 5,
        out_specs=[pl.BlockSpec(memory_space=pl.ANY)] * 4,
        scratch_shapes=[
            pltpu.VMEM(wide, low),
            pltpu.VMEM(narrow, low),
            pltpu.VMEM(narrow, low),
            pltpu.VMEM(wide, low),
            pltpu.VMEM((1, TILE), jnp.int32),
            pltpu.VMEM((2, WINDOW, WIDE), low),
            pltpu.VMEM((2 * WINDOW, WIDE), low),
            pltpu.VMEM((2 * WINDOW, HEAD_DIM), low),
            pltpu.VMEM((2, WINDOW, HEAD_DIM), low),
            pltpu.VMEM((2 * STEPS, 1, TILE), jnp.int32),
            pltpu.VMEM((HEAD_DIM, 2 * WINDOW), low),
            pltpu.VMEM((HEAD_DIM, 2 * WINDOW), low),
            pltpu.VMEM((2, SPAN, TILE), jnp.float32),
            pltpu.VMEM((2, STEPS, SPAN, TILE), low),
            pltpu.VMEM((2, STEPS, HEAD_DIM, TILE), low),
            pltpu.VMEM((2, STEPS, 1, TILE), jnp.float32),
            pltpu.VMEM((STEPS, HEAD_DIM, TILE), jnp.float32),
            pltpu.VMEM((2, WINDOW, HEAD_DIM), low),
            pltpu.VMEM((2, WINDOW, HEAD_DIM), low),
            pltpu.VMEM((2 * WINDOW, HEAD_DIM), jnp.float32),
            pltpu.VMEM((2 * WINDOW, HEAD_DIM), jnp.float32),
            pltpu.VMEM((WINDOW, HEAD_DIM), low),
            pltpu.VMEM((WINDOW, HEAD_DIM), low),
            pltpu.VMEM((WINDOW, HEAD_DIM), low),
            pltpu.VMEM((WINDOW, HEAD_DIM), low),
            pltpu.VMEM((WINDOW, HEAD_DIM), low),
            pltpu.VMEM((WINDOW, HEAD_DIM), low),
            pltpu.SemaphoreType.DMA((5,)),
            pltpu.SemaphoreType.DMA((7,)),
            pltpu.SemaphoreType.DMA((7,)),
            pltpu.SemaphoreType.DMA((11,)),
            pltpu.SemaphoreType.DMA((11,)),
            pltpu.SemaphoreType.DMA((6,)),
            pltpu.SemaphoreType.DMA((6,)),
        ],
        compiler_params=pltpu.CompilerParams(
            collective_id=0, has_side_effects=True, vmem_limit_bytes=48 * 1024 * 1024
        ),
    )(queries, keys, values, grad_out, segments)
    return pl.pallas_call(
        deliver,
        out_shape=outs,
        in_specs=[pl.BlockSpec(memory_space=pltpu.VMEM)] * 4,
        out_specs=[pl.BlockSpec(memory_space=pl.ANY)] * 4,
        scratch_shapes=[pltpu.SemaphoreType.DMA((4,))],
        compiler_params=pltpu.CompilerParams(vmem_limit_bytes=8 * 1024 * 1024),
    )(*results)


def solution(mesh):
    spec = P(("ctx", "head"), None)
    return jax.shard_map(
        body,
        mesh=mesh,
        in_specs=(spec, spec, spec, spec, P("ctx")),
        out_specs=(spec, spec, spec, spec),
        check_vma=False,
    )
```

```python
import functools
import math

import jax
import jax.numpy as jnp
from jax import lax
from jax.experimental import pallas as pl
from jax.experimental.pallas import tpu as pltpu
from jax.sharding import PartitionSpec as P

QHEADS = 32
KVHEADS = 16
HEAD_DIM = 128
WINDOW = 1024
DOCS = 8

ATTN_SCALE = 168.0 ** (-0.5)
EXP2_SCALE = ATTN_SCALE * math.log2(math.e)
MESH = pl.DeviceIdType.MESH

ROWS = 64
TILE = 256
STEPS = WINDOW // TILE
SPAN = WINDOW + TILE
HIDDEN = -1e30
APART = 2.0**17
WIDE = 2 * HEAD_DIM


def dot(a, b, dims=((1,), (0,))):
    return lax.dot_general(a, b, (dims, ((), ())), preferred_element_type=jnp.float32)


def await_bytes(ref, sem):
    pltpu.make_async_copy(ref, ref, sem).wait()


def kernel(
    q_ref, k_ref, v_ref, g_ref, seg_ref,
    a_ref, gq_ref, gk_ref, gv_ref,
    q_own, k_own, v_own, g_own, seg_own,
    qb, kb, vb, gb, segb,
    kt, vt, sb, pb, ot, inv, dq, ab, gqb, dk_acc, dv_acc, dk_out, dv_out, dk_in, dv_in, gkb, gvb,
    load, send, recv, ring_send, ring_recv, out_send, out_recv,
):
    ctx, x = lax.axis_index("ctx"), lax.axis_index("head")
    core, y, z = ctx % 2, (ctx // 2) % 4, ctx // 8
    planes = lax.axis_size("ctx") // 8
    half = y // 2
    slot = ((y % 2) * 2 + core) * 4 + x
    group = x * 4 + y
    has_after = (z < planes - 1) | (core == 0)
    has_before = (z > 0) | (core == 1)
    after = (jnp.where(core == 0, ctx + 1, ((z + 1) % planes) * 8 + y * 2), x)
    before = (jnp.where(core == 1, ctx - 1, ((z + planes - 1) % planes) * 8 + y * 2 + 1), x)
    stays = half == core
    leaves = jnp.logical_not(stays)

    def source(yy, c, dx):
        return ((z * 4 + core * 2 + yy) * 2 + c, (x + dx) % 4)

    barrier = pltpu.get_barrier_semaphore()
    for yy in range(2):
        for c in range(2):
            for dx in range(4):
                pl.semaphore_signal(barrier, inc=1, device_id=source(yy, c, dx), device_id_type=MESH)

    @pl.when(has_before)
    def _():
        pl.semaphore_signal(barrier, inc=1, device_id=before, device_id_type=MESH)

    loads = [
        pltpu.make_async_copy(src, dst, load.at[n])
        for n, (src, dst) in enumerate(
            (
                (k_ref, k_own),
                (v_ref, v_own),
                (q_ref, q_own),
                (g_ref, g_own),
                (seg_ref, seg_own),
            )
        )
    ]
    for copy in loads:
        copy.start()
    newer, older = pl.ds(WINDOW, WINDOW), pl.ds(0, WINDOW)

    @pl.when(jnp.logical_not(has_before))
    def _():
        kb[older, slice(0, HEAD_DIM)] = jnp.zeros((WINDOW, HEAD_DIM), kb.dtype)
        vb[older, :] = jnp.zeros((WINDOW, HEAD_DIM), vb.dtype)
        segb[pl.ds(0, STEPS)] = jnp.full((STEPS, 1, TILE), -1, segb.dtype)

    pl.semaphore_wait(barrier, 16 + has_after.astype(jnp.int32))

    def target(dx, dy):
        tx, ty = (x + dx) % 4, (y + dy) % 4
        return ((z * 4 + ty) * 2 + half, tx), tx * 4 + ty

    def ship(src, dst, send_sem, recv_sem, where, local):
        def far():
            pltpu.make_async_remote_copy(
                src_ref=src, dst_ref=dst, send_sem=send_sem, recv_sem=recv_sem,
                device_id=where, device_id_type=MESH,
            ).start()

        if local is None:
            far()
        else:
            pl.when(local)(lambda: pltpu.make_async_copy(src, dst, recv_sem).start())
            pl.when(jnp.logical_not(local))(far)

    offsets = [(dx, dy) for dx in range(4) for dy in range(4)]
    offsets = sorted(offsets, key=lambda o: -min(o[0], 4 - o[0]) - min(o[1], 4 - o[1]))
    own_rows = pl.ds(pl.multiple_of(slot * ROWS, ROWS), ROWS)
    own_rows2 = pl.ds(pl.multiple_of(WINDOW + slot * ROWS, ROWS), ROWS)
    loads[4].wait()
    for dy in range(4):
        where, _ = target(0, dy)
        ship(
            seg_own, segb.at[STEPS + (y % 2) * 2 + core], send.at[6], recv.at[6],
            where, stays if dy == 0 else None,
        )
    head_part, doc_part = pl.ds(0, HEAD_DIM), pl.ds(HEAD_DIM, HEAD_DIM)
    streams = (
        (k_own, kb.at[:, head_part], own_rows2, 1, 0, 0),
        (v_own, vb, own_rows2, 1, 0, 1),
        (q_own, qb.at[0, :, head_part], own_rows, 2, 0, 2),
        (q_own, qb.at[1, :, head_part], own_rows, 2, 1, None),
        (g_own, gb.at[0], own_rows, 2, 0, 3),
        (g_own, gb.at[1], own_rows, 2, 1, None),
    )
    for index, (src, dst, rows, per, n, loaded) in enumerate(streams):
        if loaded is not None:
            loads[loaded].wait()
        for dx, dy in offsets:
            where, head = target(dx, dy)
            column = (head * per + n) * HEAD_DIM
            ship(
                src.at[:, pl.ds(pl.multiple_of(column, HEAD_DIM), HEAD_DIM)],
                dst.at[rows, :],
                send.at[index],
                recv.at[index],
                where,
                stays if dx == 0 and dy == 0 else None,
            )

    ring = []
    for index, (buf, here, there) in enumerate(
        (
            (segb, pl.ds(STEPS, STEPS), pl.ds(0, STEPS)),
            (kb.at[:, head_part], newer, older),
            (vb, newer, older),
        )
    ):
        await_bytes(buf.at[here], recv.at[(6, 0, 1)[index]])
        copy = pltpu.make_async_remote_copy(
            src_ref=buf.at[here], dst_ref=buf.at[there],
            send_sem=ring_send.at[index], recv_sem=ring_recv.at[index],
            device_id=after, device_id_type=MESH,
        )
        pl.when(has_after)(copy.start)
        ring.append(copy)

    kind = lax.broadcasted_iota(jnp.int32, (HEAD_DIM, TILE), 0)

    def documents(r):
        number = segb[r]
        number = jnp.where(number < 0, DOCS, number)
        return jnp.where(kind == number, 1.0, 0.0).T

    for r in range(STEPS):
        hot = documents(STEPS + r)
        kb[pl.ds(WINDOW + r * TILE, TILE), doc_part] = hot.astype(kb.dtype)
        apart = ((hot - 1.0) * APART).astype(qb.dtype)
        for n in range(2):
            qb[n, pl.ds(r * TILE, TILE), doc_part] = apart
    kt[:, newer] = kb[newer, head_part].T
    vt[:, newer] = vb[newer, :].T
    dk_acc[...] = jnp.zeros_like(dk_acc)
    dv_acc[...] = jnp.zeros_like(dv_acc)
    pl.when(has_before)(ring[0].wait_recv)
    for r in range(STEPS):
        kb[pl.ds(r * TILE, TILE), doc_part] = documents(r).astype(kb.dtype)
    pl.when(has_before)(ring[1].wait_recv)
    kt[:, older] = kb[older, head_part].T

    key_at = lax.broadcasted_iota(jnp.int32, (TILE, TILE), 0)
    query_at = lax.broadcasted_iota(jnp.int32, (TILE, TILE), 1)

    def send_block(buf, out, per, n, index, yy, c, dx, maybe_here):
        tx, ty = (x + dx) % 4, core * 2 + yy
        ship(
            buf.at[pl.ds(pl.multiple_of(((yy * 2 + c) * 4 + tx) * ROWS, ROWS), ROWS), :],
            out.at[:, pl.ds(pl.multiple_of((group * per + n) * HEAD_DIM, HEAD_DIM), HEAD_DIM)],
            out_send.at[index],
            out_recv.at[index],
            ((z * 4 + ty) * 2 + c, tx),
            ((ty == y) & (c == core)) if maybe_here else None,
        )

    def send_back(buf, out, per, n, index):
        for dx in (2, 1, 3, 0):
            for turn in range(2):
                for c in range(2):
                    here = dx == 0 and turn == 0
                    send_block(buf, out, per, n, index, (y + turn) % 2, c, dx, here)

    def forward(n):
        def score(i, t):
            rows = pl.ds(t * TILE, TILE)
            scores = dot(
                kb[pl.ds((i + t) * TILE, TILE), :], qb[n, pl.ds(i * TILE, TILE), :], ((1,), (1,))
            )
            if t == 0:
                scores = jnp.where(key_at > query_at, scores, HIDDEN)
            if t == STEPS:
                scores = jnp.where(key_at <= query_at, scores, HIDDEN)
            sb[i % 2, rows, :] = scores
            return jnp.max(scores, axis=0, keepdims=True)

        tops = [score(0, t) for t in range(STEPS + 1)]
        for i in range(STEPS):
            top, tops, total = functools.reduce(jnp.maximum, tops), [], 0.0
            for t in range(STEPS + 1):
                rows = pl.ds(t * TILE, TILE)
                weights = jnp.exp2((sb[i % 2, rows, :] - top) * EXP2_SCALE)
                total = total + jnp.sum(weights, axis=0, keepdims=True)
                pb[n, i, rows, :] = weights.astype(jnp.bfloat16)
                if i + 1 < STEPS:
                    tops.append(score(i + 1, t))
            scale = 1.0 / total
            inv[n, i] = scale
            if n == 0 and i == 0:
                pl.when(has_before)(ring[2].wait_recv)
                vt[:, older] = vb[older, :].T
            out_t = (dot(vt[:, pl.ds(i * TILE, SPAN)], pb[n, i]) * scale).astype(jnp.bfloat16)
            ot[n, i] = out_t
            ab[n, pl.ds(i * TILE, TILE), :] = out_t.T
        send_back(ab.at[n], a_ref, 2, n, n)

    def grads_of(n, i):
        base = pl.multiple_of(i * TILE, TILE)
        grads_t = gb[n, pl.ds(base, TILE), :].T.astype(jnp.float32) * inv[n, i]
        grads_t = grads_t.astype(jnp.bfloat16)
        delta = jnp.sum(
            ot[n, i].astype(jnp.float32) * grads_t.astype(jnp.float32), axis=0, keepdims=True
        )
        return base, grads_t, delta

    def part(n, i, base, first, count, grads_t, delta):
        span = pl.ds(pl.multiple_of(base + first, TILE), count)
        weights = pb[n, i, first : first + count, :]
        prob_grads = dot(vb[span, :], grads_t)
        score_grads = (weights.astype(jnp.float32) * (prob_grads - delta)).astype(jnp.bfloat16)
        dv_acc[span, :] += dot(weights, grads_t, ((1,), (1,)))
        dk_acc[span, :] += dot(score_grads, qb[n, pl.ds(base, TILE), head_part])
        return dot(kt[:, span], score_grads)

    def finish(n, i, base, dq_t):
        gqb[n, pl.ds(base, TILE), :] = (dq_t * ATTN_SCALE).T.astype(jnp.bfloat16)

    await_bytes(qb.at[0, :, head_part], recv.at[2])
    forward(0)
    await_bytes(qb.at[1, :, head_part], recv.at[3])
    forward(1)
    await_bytes(gb.at[0], recv.at[4])

    def backward(j, carry):
        for i in (2 * j, 2 * j + 1):
            base, grads_t, delta = grads_of(0, i)
            finish(0, i, base, part(0, i, base, 0, SPAN, grads_t, delta))
        return carry

    lax.fori_loop(0, STEPS // 2, backward, 0)
    send_back(gqb.at[0], gq_ref, 2, 0, 2)
    await_bytes(gb.at[1], recv.at[5])

    def returned(b, index, src, dst):
        rows = pl.ds(pl.multiple_of(b * TILE, TILE), TILE)
        return pltpu.make_async_remote_copy(
            src_ref=src.at[rows, :], dst_ref=dst.at[rows, :],
            send_sem=ring_send.at[3 + index * STEPS + b], recv_sem=ring_recv.at[3 + index * STEPS + b],
            device_id=before, device_id_type=MESH,
        )

    for i in range(STEPS):
        dq[i] = part(1, i, i * TILE, 0, WINDOW - i * TILE, *grads_of(1, i)[1:])
        rows = pl.ds(i * TILE, TILE)
        dk_out[rows, :] = (dk_acc[rows, :] * ATTN_SCALE).astype(jnp.bfloat16)
        dv_out[rows, :] = dv_acc[rows, :].astype(jnp.bfloat16)

        @pl.when(has_before)
        def _():
            returned(i, 0, dk_out, dk_in).start()
            returned(i, 1, dv_out, dv_in).start()

    @pl.when(jnp.logical_not(has_after))
    def _():
        dk_in[...] = jnp.zeros_like(dk_in)
        dv_in[...] = jnp.zeros_like(dv_in)

    for i in range(STEPS):
        base, grads_t, delta = grads_of(1, i)
        first = WINDOW - i * TILE
        finish(1, i, base, dq[i] + part(1, i, base, first, SPAN - first, grads_t, delta))
        for dx in (2, 1, 3, 0):
            send_block(gqb.at[1], gq_ref, 2, 1, 3, i // 2, i % 2, dx, dx == 0)

    for b in range(STEPS):
        rows = pl.ds(b * TILE, TILE)
        rows_acc = pl.ds(WINDOW + b * TILE, TILE)
        for index, (acc, factor, src, came, buf, out) in enumerate(
            (
                (dk_acc, ATTN_SCALE, dk_out, dk_in, gkb, gk_ref),
                (dv_acc, 1.0, dv_out, dv_in, gvb, gv_ref),
            )
        ):
            pl.when(has_after)(returned(b, index, src, came).wait_recv)
            total = acc[rows_acc, :] * factor + came[rows, :].astype(jnp.float32)
            buf[rows, :] = total.astype(jnp.bfloat16)
            for dx in (2, 1, 3, 0):
                send_block(buf, out, 1, 0, 4 + index, b // 2, b % 2, dx, dx == 0)

    for copy in ring:
        pl.when(has_after)(copy.wait_send)

    @pl.when(has_before)
    def _():
        for b in range(STEPS):
            returned(b, 0, dk_out, dk_in).wait_send()
            returned(b, 1, dv_out, dv_in).wait_send()

    for _ in range(3):
        await_bytes(seg_own, send.at[6])
    pl.when(leaves)(functools.partial(await_bytes, seg_own, send.at[6]))
    for sems in (send, out_send):
        for index in range(6):
            await_bytes(gkb.at[pl.ds(0, 15 * ROWS), :], sems.at[index])
            pl.when(leaves)(functools.partial(await_bytes, gkb.at[pl.ds(0, ROWS), :], sems.at[index]))
    everything = pl.ds(0, KVHEADS * HEAD_DIM)
    for index, out in enumerate((a_ref, a_ref, gq_ref, gq_ref, gk_ref, gv_ref)):
        await_bytes(out.at[:, everything], out_recv.at[index])


def deliver(a_ref, gq_ref, gk_ref, gv_ref, *rest):
    outs, sem = rest[:4], rest[4]
    copies = [
        pltpu.make_async_copy(src, dst, sem.at[n])
        for n, (src, dst) in enumerate(zip((a_ref, gq_ref, gk_ref, gv_ref), outs))
    ]
    for copy in copies:
        copy.start()
    for copy in copies:
        copy.wait()


def body(queries, keys, values, grad_out, segments):
    low = jnp.bfloat16
    shape = jax.ShapeDtypeStruct
    outs = (
        shape(queries.shape, low),
        shape(queries.shape, low),
        shape(keys.shape, low),
        shape(keys.shape, low),
    )
    wide, narrow = queries.shape, keys.shape
    queries, keys, values, grad_out, segments = (
        pltpu.with_memory_space_constraint(a, pltpu.HBM)
        for a in (queries, keys, values, grad_out, segments.reshape(1, TILE))
    )
    results = pl.pallas_call(
        kernel,
        out_shape=outs,
        in_specs=[pl.BlockSpec(memory_space=pltpu.HBM)] * 5,
        out_specs=[pl.BlockSpec(memory_space=pl.ANY)] * 4,
        scratch_shapes=[
            pltpu.VMEM(wide, low),
            pltpu.VMEM(narrow, low),
            pltpu.VMEM(narrow, low),
            pltpu.VMEM(wide, low),
            pltpu.VMEM((1, TILE), jnp.int32),
            pltpu.VMEM((2, WINDOW, WIDE), low),
            pltpu.VMEM((2 * WINDOW, WIDE), low),
            pltpu.VMEM((2 * WINDOW, HEAD_DIM), low),
            pltpu.VMEM((2, WINDOW, HEAD_DIM), low),
            pltpu.VMEM((2 * STEPS, 1, TILE), jnp.int32),
            pltpu.VMEM((HEAD_DIM, 2 * WINDOW), low),
            pltpu.VMEM((HEAD_DIM, 2 * WINDOW), low),
            pltpu.VMEM((2, SPAN, TILE), jnp.float32),
            pltpu.VMEM((2, STEPS, SPAN, TILE), low),
            pltpu.VMEM((2, STEPS, HEAD_DIM, TILE), low),
            pltpu.VMEM((2, STEPS, 1, TILE), jnp.float32),
            pltpu.VMEM((STEPS, HEAD_DIM, TILE), jnp.float32),
            pltpu.VMEM((2, WINDOW, HEAD_DIM), low),
            pltpu.VMEM((2, WINDOW, HEAD_DIM), low),
            pltpu.VMEM((2 * WINDOW, HEAD_DIM), jnp.float32),
            pltpu.VMEM((2 * WINDOW, HEAD_DIM), jnp.float32),
            pltpu.VMEM((WINDOW, HEAD_DIM), low),
            pltpu.VMEM((WINDOW, HEAD_DIM), low),
            pltpu.VMEM((WINDOW, HEAD_DIM), low),
            pltpu.VMEM((WINDOW, HEAD_DIM), low),
            pltpu.VMEM((WINDOW, HEAD_DIM), low),
            pltpu.VMEM((WINDOW, HEAD_DIM), low),
            pltpu.SemaphoreType.DMA((5,)),
            pltpu.SemaphoreType.DMA((7,)),
            pltpu.SemaphoreType.DMA((7,)),
            pltpu.SemaphoreType.DMA((11,)),
            pltpu.SemaphoreType.DMA((11,)),
            pltpu.SemaphoreType.DMA((6,)),
            pltpu.SemaphoreType.DMA((6,)),
        ],
        compiler_params=pltpu.CompilerParams(
            collective_id=0, has_side_effects=True, vmem_limit_bytes=48 * 1024 * 1024
        ),
    )(queries, keys, values, grad_out, segments)
    return pl.pallas_call(
        deliver,
        out_shape=outs,
        in_specs=[pl.BlockSpec(memory_space=pltpu.VMEM)] * 4,
        out_specs=[pl.BlockSpec(memory_space=pl.ANY)] * 4,
        scratch_shapes=[pltpu.SemaphoreType.DMA((4,))],
        compiler_params=pltpu.CompilerParams(vmem_limit_bytes=8 * 1024 * 1024),
    )(*results)


def solution(mesh):
    spec = P(("ctx", "head"), None)
    return jax.shard_map(
        body,
        mesh=mesh,
        in_specs=(spec, spec, spec, spec, P("ctx")),
        out_specs=(spec, spec, spec, spec),
        check_vma=False,
    )
```

```python
import functools
import math

import jax
import jax.numpy as jnp
from jax import lax
from jax.experimental import pallas as pl
from jax.experimental.pallas import tpu as pltpu
from jax.sharding import PartitionSpec as P

QHEADS = 32
KVHEADS = 16
HEAD_DIM = 128
WINDOW = 1024
DOCS = 8

ATTN_SCALE = 168.0 ** (-0.5)
EXP2_SCALE = ATTN_SCALE * math.log2(math.e)
MESH = pl.DeviceIdType.MESH

ROWS = 64
TILE = 256
STEPS = WINDOW // TILE
SPAN = WINDOW + TILE
HIDDEN = -1e30
APART = 2.0**17
WIDE = 2 * HEAD_DIM


def dot(a, b, dims=((1,), (0,))):
    return lax.dot_general(a, b, (dims, ((), ())), preferred_element_type=jnp.float32)


def await_bytes(ref, sem):
    pltpu.make_async_copy(ref, ref, sem).wait()


def kernel(
    q_ref, k_ref, v_ref, g_ref, seg_ref,
    a_ref, gq_ref, gk_ref, gv_ref,
    q_own, k_own, v_own, g_own, seg_own,
    qb, kb, vb, gb, segb,
    kt, vt, sb, pb, ot, inv, dq, ab, gqb, dk_acc, dv_acc, dk_out, dv_out, dk_in, dv_in, gkb, gvb,
    load, send, recv, ring_send, ring_recv, out_send, out_recv,
):
    ctx, x = lax.axis_index("ctx"), lax.axis_index("head")
    core, y, z = ctx % 2, (ctx // 2) % 4, ctx // 8
    planes = lax.axis_size("ctx") // 8
    half = y // 2
    slot = ((y % 2) * 2 + core) * 4 + x
    group = x * 4 + y
    has_after = (z < planes - 1) | (core == 0)
    has_before = (z > 0) | (core == 1)
    after = (jnp.where(core == 0, ctx + 1, ((z + 1) % planes) * 8 + y * 2), x)
    before = (jnp.where(core == 1, ctx - 1, ((z + planes - 1) % planes) * 8 + y * 2 + 1), x)
    stays = half == core
    leaves = jnp.logical_not(stays)

    def source(yy, c, dx):
        return ((z * 4 + core * 2 + yy) * 2 + c, (x + dx) % 4)

    barrier = pltpu.get_barrier_semaphore()
    for dx in (2, 1, 3, 0):
        for yy in range(2):
            for c in range(2):
                pl.semaphore_signal(barrier, inc=1, device_id=source(yy, c, dx), device_id_type=MESH)

    @pl.when(has_before)
    def _():
        pl.semaphore_signal(barrier, inc=1, device_id=before, device_id_type=MESH)

    loads = [
        pltpu.make_async_copy(src, dst, load.at[n])
        for n, (src, dst) in enumerate(
            (
                (k_ref, k_own),
                (v_ref, v_own),
                (q_ref, q_own),
                (g_ref, g_own),
                (seg_ref, seg_own),
            )
        )
    ]
    for copy in loads:
        copy.start()
    newer, older = pl.ds(WINDOW, WINDOW), pl.ds(0, WINDOW)

    @pl.when(jnp.logical_not(has_before))
    def _():
        kb[older, slice(0, HEAD_DIM)] = jnp.zeros((WINDOW, HEAD_DIM), kb.dtype)
        vb[older, :] = jnp.zeros((WINDOW, HEAD_DIM), vb.dtype)
        segb[pl.ds(0, STEPS)] = jnp.full((STEPS, 1, TILE), -1, segb.dtype)

    pl.semaphore_wait(barrier, 16 + has_after.astype(jnp.int32))

    def target(dx, dy):
        tx, ty = (x + dx) % 4, (y + dy) % 4
        return ((z * 4 + ty) * 2 + half, tx), tx * 4 + ty

    def ship(src, dst, send_sem, recv_sem, where, local):
        def far():
            pltpu.make_async_remote_copy(
                src_ref=src, dst_ref=dst, send_sem=send_sem, recv_sem=recv_sem,
                device_id=where, device_id_type=MESH,
            ).start()

        if local is None:
            far()
        else:
            pl.when(local)(lambda: pltpu.make_async_copy(src, dst, recv_sem).start())
            pl.when(jnp.logical_not(local))(far)

    offsets = (
        (2, 2), (2, 1), (1, 2), (2, 3), (3, 2), (1, 1), (3, 3), (1, 3),
        (3, 1), (2, 0), (0, 2), (1, 0), (3, 0), (0, 1), (0, 3), (0, 0),
    )
    own_rows = pl.ds(pl.multiple_of(slot * ROWS, ROWS), ROWS)
    own_rows2 = pl.ds(pl.multiple_of(WINDOW + slot * ROWS, ROWS), ROWS)
    loads[4].wait()
    for dy in range(4):
        where, _ = target(0, dy)
        ship(
            seg_own, segb.at[STEPS + (y % 2) * 2 + core], send.at[6], recv.at[6],
            where, stays if dy == 0 else None,
        )
    head_part, doc_part = pl.ds(0, HEAD_DIM), pl.ds(HEAD_DIM, HEAD_DIM)
    streams = (
        (k_own, kb.at[:, head_part], own_rows2, 1, 0, 0),
        (v_own, vb, own_rows2, 1, 0, 1),
        (q_own, qb.at[0, :, head_part], own_rows, 2, 0, 2),
        (q_own, qb.at[1, :, head_part], own_rows, 2, 1, None),
        (g_own, gb.at[0], own_rows, 2, 0, 3),
        (g_own, gb.at[1], own_rows, 2, 1, None),
    )
    for index, (src, dst, rows, per, n, loaded) in enumerate(streams):
        if loaded is not None:
            loads[loaded].wait()
        for dx, dy in offsets:
            where, head = target(dx, dy)
            column = (head * per + n) * HEAD_DIM
            ship(
                src.at[:, pl.ds(pl.multiple_of(column, HEAD_DIM), HEAD_DIM)],
                dst.at[rows, :],
                send.at[index],
                recv.at[index],
                where,
                stays if dx == 0 and dy == 0 else None,
            )

    ring = []
    for index, (buf, here, there) in enumerate(
        (
            (segb, pl.ds(STEPS, STEPS), pl.ds(0, STEPS)),
            (kb.at[:, head_part], newer, older),
            (vb, newer, older),
        )
    ):
        await_bytes(buf.at[here], recv.at[(6, 0, 1)[index]])
        copy = pltpu.make_async_remote_copy(
            src_ref=buf.at[here], dst_ref=buf.at[there],
            send_sem=ring_send.at[index], recv_sem=ring_recv.at[index],
            device_id=after, device_id_type=MESH,
        )
        pl.when(has_after)(copy.start)
        ring.append(copy)

    kind = lax.broadcasted_iota(jnp.int32, (HEAD_DIM, TILE), 0)

    def documents(r):
        number = segb[r]
        number = jnp.where(number < 0, DOCS, number)
        return jnp.where(kind == number, 1.0, 0.0).T

    for r in range(STEPS):
        hot = documents(STEPS + r)
        kb[pl.ds(WINDOW + r * TILE, TILE), doc_part] = hot.astype(kb.dtype)
        apart = ((hot - 1.0) * APART).astype(qb.dtype)
        for n in range(2):
            qb[n, pl.ds(r * TILE, TILE), doc_part] = apart
    kt[:, newer] = kb[newer, head_part].T
    vt[:, newer] = vb[newer, :].T
    dk_acc[...] = jnp.zeros_like(dk_acc)
    dv_acc[...] = jnp.zeros_like(dv_acc)
    pl.when(has_before)(ring[0].wait_recv)
    for r in range(STEPS):
        kb[pl.ds(r * TILE, TILE), doc_part] = documents(r).astype(kb.dtype)
    pl.when(has_before)(ring[1].wait_recv)
    kt[:, older] = kb[older, head_part].T

    key_at = lax.broadcasted_iota(jnp.int32, (TILE, TILE), 0)
    query_at = lax.broadcasted_iota(jnp.int32, (TILE, TILE), 1)

    def send_block(buf, out, per, n, index, yy, c, dx, maybe_here):
        tx, ty = (x + dx) % 4, core * 2 + yy
        ship(
            buf.at[pl.ds(pl.multiple_of(((yy * 2 + c) * 4 + tx) * ROWS, ROWS), ROWS), :],
            out.at[:, pl.ds(pl.multiple_of((group * per + n) * HEAD_DIM, HEAD_DIM), HEAD_DIM)],
            out_send.at[index],
            out_recv.at[index],
            ((z * 4 + ty) * 2 + c, tx),
            ((ty == y) & (c == core)) if maybe_here else None,
        )

    def send_back(buf, out, per, n, index):
        for dx in (2, 1, 3, 0):
            for turn in range(2):
                for c in range(2):
                    here = dx == 0 and turn == 0
                    send_block(buf, out, per, n, index, (y + turn) % 2, c, dx, here)

    def forward(n):
        def score(i, t):
            rows = pl.ds(t * TILE, TILE)
            scores = dot(
                kb[pl.ds((i + t) * TILE, TILE), :], qb[n, pl.ds(i * TILE, TILE), :], ((1,), (1,))
            )
            if t == 0:
                scores = jnp.where(key_at > query_at, scores, HIDDEN)
            if t == STEPS:
                scores = jnp.where(key_at <= query_at, scores, HIDDEN)
            sb[i % 2, rows, :] = scores
            return jnp.max(scores, axis=0, keepdims=True)

        tops = [score(0, t) for t in range(STEPS + 1)]
        for i in range(STEPS):
            top, tops, total = functools.reduce(jnp.maximum, tops), [], 0.0
            for t in range(STEPS + 1):
                rows = pl.ds(t * TILE, TILE)
                weights = jnp.exp2((sb[i % 2, rows, :] - top) * EXP2_SCALE)
                total = total + jnp.sum(weights, axis=0, keepdims=True)
                pb[n, i, rows, :] = weights.astype(jnp.bfloat16)
                if i + 1 < STEPS:
                    tops.append(score(i + 1, t))
            scale = 1.0 / total
            inv[n, i] = scale
            if n == 0 and i == 0:
                pl.when(has_before)(ring[2].wait_recv)
                vt[:, older] = vb[older, :].T
            out_t = (dot(vt[:, pl.ds(i * TILE, SPAN)], pb[n, i]) * scale).astype(jnp.bfloat16)
            ot[n, i] = out_t
            ab[n, pl.ds(i * TILE, TILE), :] = out_t.T
        send_back(ab.at[n], a_ref, 2, n, n)

    def grads_of(n, i):
        base = pl.multiple_of(i * TILE, TILE)
        grads_t = gb[n, pl.ds(base, TILE), :].T.astype(jnp.float32) * inv[n, i]
        grads_t = grads_t.astype(jnp.bfloat16)
        delta = jnp.sum(
            ot[n, i].astype(jnp.float32) * grads_t.astype(jnp.float32), axis=0, keepdims=True
        )
        return base, grads_t, delta

    def part(n, i, base, first, count, grads_t, delta):
        span = pl.ds(pl.multiple_of(base + first, TILE), count)
        weights = pb[n, i, first : first + count, :]
        prob_grads = dot(vb[span, :], grads_t)
        score_grads = (weights.astype(jnp.float32) * (prob_grads - delta)).astype(jnp.bfloat16)
        dv_acc[span, :] += dot(weights, grads_t, ((1,), (1,)))
        dk_acc[span, :] += dot(score_grads, qb[n, pl.ds(base, TILE), head_part])
        return dot(kt[:, span], score_grads)

    def finish(n, i, base, dq_t):
        gqb[n, pl.ds(base, TILE), :] = (dq_t * ATTN_SCALE).T.astype(jnp.bfloat16)

    await_bytes(qb.at[0, :, head_part], recv.at[2])
    forward(0)
    await_bytes(qb.at[1, :, head_part], recv.at[3])
    forward(1)
    await_bytes(gb.at[0], recv.at[4])

    def backward(j, carry):
        for i in (2 * j, 2 * j + 1):
            base, grads_t, delta = grads_of(0, i)
            finish(0, i, base, part(0, i, base, 0, SPAN, grads_t, delta))
        return carry

    lax.fori_loop(0, STEPS // 2, backward, 0)
    send_back(gqb.at[0], gq_ref, 2, 0, 2)
    await_bytes(gb.at[1], recv.at[5])

    def returned(b, index, src, dst):
        rows = pl.ds(pl.multiple_of(b * TILE, TILE), TILE)
        return pltpu.make_async_remote_copy(
            src_ref=src.at[rows, :], dst_ref=dst.at[rows, :],
            send_sem=ring_send.at[3 + index * STEPS + b], recv_sem=ring_recv.at[3 + index * STEPS + b],
            device_id=before, device_id_type=MESH,
        )

    for i in range(STEPS):
        dq[i] = part(1, i, i * TILE, 0, WINDOW - i * TILE, *grads_of(1, i)[1:])
        rows = pl.ds(i * TILE, TILE)
        dk_out[rows, :] = (dk_acc[rows, :] * ATTN_SCALE).astype(jnp.bfloat16)
        dv_out[rows, :] = dv_acc[rows, :].astype(jnp.bfloat16)

        @pl.when(has_before)
        def _():
            returned(i, 0, dk_out, dk_in).start()
            returned(i, 1, dv_out, dv_in).start()

    @pl.when(jnp.logical_not(has_after))
    def _():
        dk_in[...] = jnp.zeros_like(dk_in)
        dv_in[...] = jnp.zeros_like(dv_in)

    for i in range(STEPS):
        base, grads_t, delta = grads_of(1, i)
        first = WINDOW - i * TILE
        finish(1, i, base, dq[i] + part(1, i, base, first, SPAN - first, grads_t, delta))
        for dx in (2, 1, 3, 0):
            send_block(gqb.at[1], gq_ref, 2, 1, 3, i // 2, i % 2, dx, dx == 0)

    for b in range(STEPS):
        rows = pl.ds(b * TILE, TILE)
        rows_acc = pl.ds(WINDOW + b * TILE, TILE)
        for index, (acc, factor, src, came, buf, out) in enumerate(
            (
                (dk_acc, ATTN_SCALE, dk_out, dk_in, gkb, gk_ref),
                (dv_acc, 1.0, dv_out, dv_in, gvb, gv_ref),
            )
        ):
            pl.when(has_after)(returned(b, index, src, came).wait_recv)
            total = acc[rows_acc, :] * factor + came[rows, :].astype(jnp.float32)
            buf[rows, :] = total.astype(jnp.bfloat16)
            for dx in (2, 1, 3, 0):
                send_block(buf, out, 1, 0, 4 + index, b // 2, b % 2, dx, dx == 0)

    for copy in ring:
        pl.when(has_after)(copy.wait_send)

    @pl.when(has_before)
    def _():
        for b in range(STEPS):
            returned(b, 0, dk_out, dk_in).wait_send()
            returned(b, 1, dv_out, dv_in).wait_send()

    for _ in range(3):
        await_bytes(seg_own, send.at[6])
    pl.when(leaves)(functools.partial(await_bytes, seg_own, send.at[6]))
    for sems in (send, out_send):
        for index in range(6):
            await_bytes(gkb.at[pl.ds(0, 15 * ROWS), :], sems.at[index])
            pl.when(leaves)(functools.partial(await_bytes, gkb.at[pl.ds(0, ROWS), :], sems.at[index]))
    everything = pl.ds(0, KVHEADS * HEAD_DIM)
    for index, out in enumerate((a_ref, a_ref, gq_ref, gq_ref, gk_ref, gv_ref)):
        await_bytes(out.at[:, everything], out_recv.at[index])


def deliver(a_ref, gq_ref, gk_ref, gv_ref, *rest):
    outs, sem = rest[:4], rest[4]
    copies = [
        pltpu.make_async_copy(src, dst, sem.at[n])
        for n, (src, dst) in enumerate(zip((a_ref, gq_ref, gk_ref, gv_ref), outs))
    ]
    for copy in copies:
        copy.start()
    for copy in copies:
        copy.wait()


def body(queries, keys, values, grad_out, segments):
    low = jnp.bfloat16
    shape = jax.ShapeDtypeStruct
    outs = (
        shape(queries.shape, low),
        shape(queries.shape, low),
        shape(keys.shape, low),
        shape(keys.shape, low),
    )
    wide, narrow = queries.shape, keys.shape
    queries, keys, values, grad_out, segments = (
        pltpu.with_memory_space_constraint(a, pltpu.HBM)
        for a in (queries, keys, values, grad_out, segments.reshape(1, TILE))
    )
    results = pl.pallas_call(
        kernel,
        out_shape=outs,
        in_specs=[pl.BlockSpec(memory_space=pltpu.HBM)] * 5,
        out_specs=[pl.BlockSpec(memory_space=pl.ANY)] * 4,
        scratch_shapes=[
            pltpu.VMEM(wide, low),
            pltpu.VMEM(narrow, low),
            pltpu.VMEM(narrow, low),
            pltpu.VMEM(wide, low),
            pltpu.VMEM((1, TILE), jnp.int32),
            pltpu.VMEM((2, WINDOW, WIDE), low),
            pltpu.VMEM((2 * WINDOW, WIDE), low),
            pltpu.VMEM((2 * WINDOW, HEAD_DIM), low),
            pltpu.VMEM((2, WINDOW, HEAD_DIM), low),
            pltpu.VMEM((2 * STEPS, 1, TILE), jnp.int32),
            pltpu.VMEM((HEAD_DIM, 2 * WINDOW), low),
            pltpu.VMEM((HEAD_DIM, 2 * WINDOW), low),
            pltpu.VMEM((2, SPAN, TILE), jnp.float32),
            pltpu.VMEM((2, STEPS, SPAN, TILE), low),
            pltpu.VMEM((2, STEPS, HEAD_DIM, TILE), low),
            pltpu.VMEM((2, STEPS, 1, TILE), jnp.float32),
            pltpu.VMEM((STEPS, HEAD_DIM, TILE), jnp.float32),
            pltpu.VMEM((2, WINDOW, HEAD_DIM), low),
            pltpu.VMEM((2, WINDOW, HEAD_DIM), low),
            pltpu.VMEM((2 * WINDOW, HEAD_DIM), jnp.float32),
            pltpu.VMEM((2 * WINDOW, HEAD_DIM), jnp.float32),
            pltpu.VMEM((WINDOW, HEAD_DIM), low),
            pltpu.VMEM((WINDOW, HEAD_DIM), low),
            pltpu.VMEM((WINDOW, HEAD_DIM), low),
            pltpu.VMEM((WINDOW, HEAD_DIM), low),
            pltpu.VMEM((WINDOW, HEAD_DIM), low),
            pltpu.VMEM((WINDOW, HEAD_DIM), low),
            pltpu.SemaphoreType.DMA((5,)),
            pltpu.SemaphoreType.DMA((7,)),
            pltpu.SemaphoreType.DMA((7,)),
            pltpu.SemaphoreType.DMA((11,)),
            pltpu.SemaphoreType.DMA((11,)),
            pltpu.SemaphoreType.DMA((6,)),
            pltpu.SemaphoreType.DMA((6,)),
        ],
        compiler_params=pltpu.CompilerParams(
            collective_id=0, has_side_effects=True, vmem_limit_bytes=48 * 1024 * 1024
        ),
    )(queries, keys, values, grad_out, segments)
    return pl.pallas_call(
        deliver,
        out_shape=outs,
        in_specs=[pl.BlockSpec(memory_space=pltpu.VMEM)] * 4,
        out_specs=[pl.BlockSpec(memory_space=pl.ANY)] * 4,
        scratch_shapes=[pltpu.SemaphoreType.DMA((4,))],
        compiler_params=pltpu.CompilerParams(vmem_limit_bytes=8 * 1024 * 1024),
    )(*results)


def solution(mesh):
    spec = P(("ctx", "head"), None)
    return jax.shard_map(
        body,
        mesh=mesh,
        in_specs=(spec, spec, spec, spec, P("ctx")),
        out_specs=(spec, spec, spec, spec),
        check_vma=False,
    )
```
